32 devices in a mesh: row: 8 (over y, x, core), col: 4 (over z).
Axes of the slice: x: 2, y: 2, z: 4, core: 2. Of those that a mesh axis runs over, the one named last changes fastest.
Arguments:
- right_side: float32 [2, 2048, 1024], P(None, 'row', 'col'), may hold values from -6 to 6
- probe: float32 [2, 256, 256], replicated, may hold values from -6 to 6
- detector_weights: float32 [256, 256], replicated, may hold values from 0.1 to 10
- offsets: int32 [8, 4, 4, 2], P('row', 'col'), may hold values from -128 to 127, as said below
- counts: int32 [8, 4], P('row', 'col'), may hold values from 2 to 4, as said below
Outputs:
- solution_field: float32 [2, 2048, 1024], P(None, 'row', 'col')
- residual: float32 [2, 2048, 1024], P(None, 'row', 'col')
The draws below stay inside these ranges and needn't reach their ends.
Inputs may be any that keep to these rules, and one draw needn't show every extreme that they name: `counts`: every region holds at least two positions; in every draw some region holds exactly 4. In every region slot 0 has both offsets negative and slot 1 both offsets non-negative.
All inputs are finite; a program needn't handle non-finite values.
Results may differ from the reference program's by a relative error of at most 0.0003.
Values sent between devices are 32-bit elements; how exact they have to be, the bound alone decides.
A program may use at most 64 MiB of HBM per device.

```python
import math
import jax
import jax.numpy as jnp
from jax import lax

PATCH = 256
CAP = 4
ITERS = 3
NY = 2048
NX = 1024
N_ROW = 8
N_COL = 4


def draw_counts(key, part):
    key_full, key_low, key_pick = jax.random.split(jax.random.fold_in(key, 71), 3)
    heavy = jax.random.randint(key_full, (N_ROW, N_COL), 0, 4) == 0
    light = jax.random.randint(key_low, (N_ROW, N_COL), 2, max(CAP // 2, 2) + 1)
    filled = jnp.where(heavy, CAP, light).reshape(-1)
    chosen = jax.random.randint(key_pick, (), 0, N_ROW * N_COL)
    filled = filled.at[chosen].set(CAP)
    return filled.reshape(N_ROW, N_COL).astype(jnp.int32)


def draw_offsets(key, part):
    half = PATCH // 2
    key_rest, key_low, key_high = jax.random.split(jax.random.fold_in(key, 53), 3)
    rest = jax.random.randint(key_rest, (N_ROW, N_COL, CAP, 2), -half, half)
    low = jax.random.randint(key_low, (N_ROW, N_COL, 1, 2), -half, 0)
    high = jax.random.randint(key_high, (N_ROW, N_COL, 1, 2), 0, half)
    return jnp.concatenate([low, high, rest[:, :, 2:]], axis=2).astype(jnp.int32)


def shard_levels(stream_key, extent, shards, least, high):
    def one(position, blocks):
        draws = jax.random.uniform(jax.random.fold_in(jax.random.fold_in(stream_key, 6), position), (blocks,), jnp.float32, least / len(shards), high / len(shards))
        return jnp.repeat(jnp.exp(draws), extent[position] // blocks).reshape((-1,) + (1,) * (len(extent) - position - 1))

    gain = one(*shards[0])
    for cut in shards[1:]:
        gain = gain * one(*cut)
    return gain


def centred(own_key, shape, spread, bound, cuts=(), held_as=jnp.bfloat16):
    drawn = jax.random.normal(own_key, shape, jnp.float32) * spread
    if len(cuts) > 0:
        drawn = shard_levels(own_key, shape, cuts, -0.22, 0.18) * drawn
    return jnp.clip(drawn, min=-bound, max=bound).astype(held_as)


def setup_inputs(seed: int = 0) -> dict:
    arg_keys = jax.random.split(jax.random.key(seed), 6)
    return {
        "right_side": centred(arg_keys[0], (2, NY, NX), 1.0, 6.0, ((1, 8), (2, 4)), jnp.float32),
        "probe": centred(arg_keys[1], (2, PATCH, PATCH), 1.0, 6.0, (), jnp.float32),
        "detector_weights": jnp.clip(jnp.exp(jax.random.uniform(arg_keys[2], (PATCH, PATCH), jnp.float32, math.log(0.1), math.log(10.0))), 0.1, 10.0),
        "offsets": draw_offsets(jax.random.fold_in(arg_keys[5], 71), 0),
        "counts": draw_counts(jax.random.fold_in(arg_keys[5], 71), 0),
    }


ridge_weight = 0.5


def patch_normal(tile_in, probe, weights):
    illum = lax.complex(probe[0], probe[1])
    wave = illum * lax.complex(tile_in[0], tile_in[1])
    freq = jnp.fft.fft2(wave, norm="ortho")
    back = jnp.fft.ifft2(freq * weights, norm="ortho")
    result = jnp.conj(illum) * back
    return jnp.stack([jnp.real(result), jnp.imag(result)])


def operate(field, probe, weights, row_starts, col_starts, weight_on):
    margin = PATCH // 2
    padded = jnp.pad(field, ((0, 0), (margin, margin), (margin, margin)))

    def visit(summed, item):
        row_at, col_at, flag = item
        zero_idx = jnp.zeros((), jnp.int32)
        tile_in = lax.dynamic_slice(padded, (zero_idx, row_at, col_at), (2, PATCH, PATCH))
        update = patch_normal(tile_in, probe, weights) * flag
        current = lax.dynamic_slice(summed, (zero_idx, row_at, col_at), (2, PATCH, PATCH))
        return lax.dynamic_update_slice(summed, current + update, (zero_idx, row_at, col_at)), None

    summed, _ = lax.scan(visit, jnp.zeros_like(padded), (row_starts, col_starts, weight_on))
    return summed[:, margin:margin + NY, margin:margin + NX] + ridge_weight * field


def inner(first, second):
    return jnp.sum(first * second)


def reference(right_side, probe, detector_weights, offsets, counts):
    margin = PATCH // 2
    region_row = (jnp.arange(N_ROW, dtype=jnp.int32) * PATCH + margin)[:, None, None]
    region_col = (jnp.arange(N_COL, dtype=jnp.int32) * PATCH + margin)[None, :, None]
    row_starts = (offsets[:, :, :, 0].astype(jnp.int32) + region_row).reshape(-1).astype(jnp.int32)
    col_starts = (offsets[:, :, :, 1].astype(jnp.int32) + region_col).reshape(-1).astype(jnp.int32)
    slot_ids = jnp.arange(CAP, dtype=jnp.int32)[None, None, :]
    weight_on = (slot_ids < counts[:, :, None]).astype(jnp.float32).reshape(-1)
    solution_field = jnp.zeros_like(right_side)
    residual, direction = right_side, right_side
    norm_now = inner(residual, residual)
    for iteration in range(ITERS):
        image = operate(direction, probe, detector_weights, row_starts, col_starts, weight_on)
        alpha = norm_now / inner(direction, image)
        solution_field = solution_field + alpha * direction
        residual = residual - alpha * image
        norm_next = inner(residual, residual)
        direction = residual + (norm_next / norm_now) * direction
        norm_now = norm_next
    return solution_field, residual
```

```python
import functools
import math

import jax
import jax.numpy as jnp
import numpy as np
from jax import lax
from jax.experimental import pallas as pl
from jax.experimental.pallas import tpu as pltpu
from jax.sharding import PartitionSpec as P

ITERS = 3
RIDGE = 0.5
SKEW = 4.5
MESH = pl.DeviceIdType.MESH
F32 = jnp.float32
BF16 = jnp.bfloat16


def tables(length):
    half = length // 2
    k = np.arange(half)[:, None]
    n = np.arange(half)[None, :]
    out = []
    for odd in (0, 1):
        angle = 2.0 * math.pi * ((n * (2 * k + odd)) % length) / length
        re, im = np.cos(angle) / math.sqrt(length), -np.sin(angle) / math.sqrt(length)
        real = np.block([[re, -im], [im, re]])
        for mat in (real, real.T):
            hi = mat.astype(BF16)
            out += [hi, (mat - hi.astype(np.float64)).astype(BF16)]
    return np.stack(out)


def kernel(
    n_row, n_col, cap, side,
    off_ref, cnt_ref, rhs_hbm, probe_hbm, w_hbm, mat_hbm,
    SOL, res_ref,
    R, G, L, S, D, PR, P0, W0, mat_ref, XA, XB, YA, YB, W, RA, CA, CC, RC, T1, T2,
    bar_send, bar_recv, s1_send, s1_recv, s2_send, s2_recv, io_sem,
):
    h = side // 2
    own = slice(h, h + side)
    row = lax.axis_index("row")
    col = lax.axis_index("col")

    load_r = pltpu.make_async_copy(rhs_hbm, R.at[:, own, own], io_sem.at[0])
    load_p = pltpu.make_async_copy(probe_hbm, P0, io_sem.at[1])
    load_w = pltpu.make_async_copy(w_hbm, W0, io_sem.at[2])
    load_m = pltpu.make_async_copy(mat_hbm, mat_ref, io_sem.at[3])
    for load in (load_r, load_p, load_w, load_m):
        load.start()

    def chunks(total, step, body):
        def run(i, carry):
            body(pl.ds(pl.multiple_of(i * step, step), step))
            return carry
        lax.fori_loop(0, total // step, run, 0)

    def fill(buf, rows, cols):
        def run(i, carry):
            at = pl.ds(pl.multiple_of(rows.start + i * 32, 32), 32)
            buf[:, at, cols] = jnp.zeros((2, 32, cols.stop - cols.start), F32)
            return carry
        lax.fori_loop(0, (rows.stop - rows.start) // 32, run, 0)

    every = slice(0, 2 * side)
    for rows in (slice(0, h), slice(3 * h, 4 * h)):
        fill(R, rows, every)
    for cols in (slice(0, h), slice(3 * h, 4 * h)):
        fill(R, own, cols)
    for buf in (RA, CA, CC, RC):
        fill(buf, slice(0, buf.shape[1]), slice(0, buf.shape[2]))
    barrier = pltpu.get_barrier_semaphore()
    for d in range(1, n_row):
        pl.semaphore_signal(barrier, inc=1, device_id=(lax.rem(row + d, n_row), col), device_id_type=MESH)
    for d in range(1, n_col):
        pl.semaphore_signal(barrier, inc=1, device_id=(row, lax.rem(col + d, n_col)), device_id_type=MESH)
    pl.semaphore_wait(barrier, n_row - 1 + n_col - 1)

    def both(index, low_src, low_dst, high_src, high_dst, axis):
        at, count = (row, n_row) if axis == 0 else (col, n_col)

        def target(step):
            return (row + step, col) if axis == 0 else (row, col + step)

        low = pltpu.make_async_remote_copy(
            src_ref=low_src, dst_ref=low_dst, send_sem=bar_send.at[2 * index], recv_sem=bar_recv.at[2 * index],
            device_id=target(-1), device_id_type=MESH)
        high = pltpu.make_async_remote_copy(
            src_ref=high_src, dst_ref=high_dst, send_sem=bar_send.at[2 * index + 1],
            recv_sem=bar_recv.at[2 * index + 1], device_id=target(1), device_id_type=MESH)

        def start():
            pl.when(at > 0)(low.start)
            pl.when(at < count - 1)(high.start)

        def wait():
            @pl.when(at > 0)
            def _():
                low.wait_send()
                high.wait_recv()

            @pl.when(at < count - 1)
            def _():
                high.wait_send()
                low.wait_recv()

        return start, wait

    edges = (slice(0, h), slice(3 * h, 4 * h))
    one, two, top_h, end_h = slice(h, 2 * h), slice(2 * h, 3 * h), slice(0, h), slice(3 * h, 4 * h)

    def gather(F):
        re_turn = both(8, F.at[0, own, one], F.at[0, own, end_h], F.at[0, own, two], F.at[0, own, top_h], 1)
        im_turn = both(9, F.at[1, one, own], F.at[1, end_h, own], F.at[1, two, own], F.at[1, top_h, own], 0)
        rest = [
            both(10, F.at[0, one, own], F.at[0, end_h, own], F.at[0, two, own], F.at[0, top_h, own], 0),
            both(11, F.at[1, own, one], F.at[1, own, end_h], F.at[1, own, two], F.at[1, own, top_h], 1),
        ]
        for start, _ in (re_turn, im_turn, *rest):
            start()
        re_turn[1]()
        for q, e in enumerate(edges):
            rest.append(both(12 + q, F.at[0, one, e], F.at[0, end_h, e], F.at[0, two, e], F.at[0, top_h, e], 0))
            rest[-1][0]()
        im_turn[1]()
        for q, e in enumerate(edges):
            rest.append(both(14 + q, F.at[1, e, one], F.at[1, e, end_h], F.at[1, e, two], F.at[1, e, top_h], 1))
            rest[-1][0]()

        def wait():
            for _, done in rest:
                done()

        return wait

    load_r.wait()
    gather_wait = gather(R)

    fill(G, every, every)
    fill(L, every, every)
    for buf in (D, SOL):
        fill(buf, slice(0, buf.shape[1]), slice(0, buf.shape[2]))

    load_p.wait()
    for s in range(cap):
        on = jnp.where(s < cnt_ref[0, 0], 1.0, 0.0).astype(F32)
        for c in range(2):
            rolled = pltpu.roll(P0[c], off_ref[0, s] + h, 0)
            PR[s, c] = pltpu.roll(rolled, off_ref[1, s] + h, 1) * on

    def three(val):
        top = val.astype(BF16)
        rest = val - top.astype(F32)
        mid = rest.astype(BF16)
        return top, mid, (rest - mid.astype(F32)).astype(BF16)

    load_w.wait()
    first = lax.broadcasted_iota(jnp.int32, (side, side), 0)
    second = lax.broadcasted_iota(jnp.int32, (side, side), 1)
    freq = jnp.where(first >= h, 2 * (first - h) + 1, 2 * first)
    pick = jnp.where(second == freq, 1.0, 0.0).astype(BF16)
    by_row = sum(jnp.dot(pick, part, preferred_element_type=F32) for part in three(W0[...]))
    parts = three(by_row)
    lane = jnp.where(second >= h, second - h, second)
    for q in range(2):
        pick = jnp.where(first == 2 * lane + q, 1.0, 0.0).astype(BF16)
        W[q] = sum(jnp.dot(part, pick, preferred_element_type=F32) for part in parts)

    load_m.wait()
    gather_wait()

    step = 32

    def fold(val):
        return jnp.sum(val.reshape(-1, 8, val.shape[-1]), axis=0)

    sub = lax.broadcasted_iota(jnp.int32, (step, h), 0)
    lan = lax.broadcasted_iota(jnp.int32, (step, h), 1)

    def side_of(s, at):
        if s == 0:
            return "both" if at < h else "near"
        if s == 1:
            return "far" if at < h else "both"
        return "both"

    def patch(s, k, seen, acc):
        X, Y = (XA, YA) if k == 0 else (XB, YB)
        a = off_ref[0, s] + h
        b = off_ref[1, s] + h

        def put(j, rows, val):
            hi = val.astype(BF16)
            X[j, 0, rows, :] = hi
            X[j, 1, rows, :] = (val - hi.astype(F32)).astype(BF16)

        def left(m, j):
            hi, lo = mat_ref[m], mat_ref[m + 1]
            xh, xl = X[j, 0], X[j, 1]
            return jnp.dot(
                jnp.concatenate([hi, lo, hi], 1), jnp.concatenate([xh, xh, xl], 0), preferred_element_type=F32)

        def right(j, m):
            hi, lo = mat_ref[m], mat_ref[m + 1]
            xh, xl = X[j, 0], X[j, 1]
            return jnp.dot(
                jnp.concatenate([xh, xl, xh], 1), jnp.concatenate([hi, hi, lo], 0), preferred_element_type=F32)

        def covered(c, base):
            halves = []
            for at in (0, h):
                cols, fcols = slice(at, at + h), slice(side + at, side + at + h)
                rk, ck = side_of(s, base), side_of(s, at)
                rows, far = slice(base, base + step), slice(side + base, side + base + step)

                def in_cols(r):
                    if ck == "near":
                        return R[c, r, cols]
                    if ck == "far":
                        return R[c, r, fcols]
                    return jnp.where(lan + at >= b, R[c, r, cols], R[c, r, fcols])

                if rk == "near":
                    halves.append(in_cols(rows))
                elif rk == "far":
                    halves.append(in_cols(far))
                else:
                    halves.append(jnp.where(sub + base >= a, in_cols(rows), in_cols(far)))
            return jnp.concatenate(halves, 1)

        def scatter(c, base, term):
            for at in (0, h):
                val = term[:, at:at + h]
                rk, ck = side_of(s, base), side_of(s, at)
                rows = {}
                if rk == "both":
                    near = jnp.where(sub + base >= a, val, 0.0)
                    rows = {0: near, side: val - near}
                else:
                    rows = {0 if rk == "near" else side: val}
                for shift, part in rows.items():
                    if ck == "both":
                        near = jnp.where(lan + at >= b, part, 0.0)
                        cells = {0: near, side: part - near}
                    else:
                        cells = {0 if ck == "near" else side: part}
                    for over, cell in cells.items():
                        r0, c0 = shift + base, over + at
                        where = (c, slice(r0, r0 + step), slice(c0, c0 + h))
                        if (c, r0, c0) in seen:
                            S[where] += cell
                        else:
                            S[where] = cell
                            seen.add((c, r0, c0))

        def load():
            for t in range(0, h, step):
                parts = []
                for base in (t, h + t):
                    rows = slice(base, base + step)
                    v = [covered(c, base) for c in range(2)]
                    p0, p1 = PR[s, 0, rows, :], PR[s, 1, rows, :]
                    parts.append((p0 * v[0] - p1 * v[1], p0 * v[1] + p1 * v[0]))
                for c in range(2):
                    rows = slice(c * h + t, c * h + t + step)
                    put(0, rows, parts[0][c] + parts[1][c])
                    put(1, rows, parts[0][c] - parts[1][c])

        def mul_a():
            Y[0] = left(0, 0)
            Y[1] = left(4, 1)

        def mix_b():
            for j in range(2):
                for t in range(0, h, step):
                    re, im = Y[j, t:t + step, :], Y[j, h + t:h + t + step, :]
                    rows = slice(j * h + t, j * h + t + step)
                    put(2, rows, jnp.concatenate([re[:, :h] + re[:, h:], im[:, :h] + im[:, h:]], 1))
                    put(3, rows, jnp.concatenate([re[:, :h] - re[:, h:], im[:, :h] - im[:, h:]], 1))

        def mul_b():
            Y[2] = right(2, 2)
            Y[3] = right(3, 6)

        def mix_c():
            for j in range(2):
                for t in range(0, side, step):
                    rows = slice(t, t + step)
                    f = Y[2 + j, rows, :]
                    wf = W[j, rows, :] * f
                    acc[0] = acc[0] + fold(wf * f)
                    put(j, rows, wf)

        def mul_c():
            Y[0] = right(0, 0)
            Y[1] = right(1, 4)

        def mix_d():
            for j in range(2):
                for t in range(0, h, step):
                    rows = slice(j * h + t, j * h + t + step)
                    c, d = Y[0, rows, :], Y[1, rows, :]
                    p, m = c + d, c - d
                    put(2 + j, slice(t, t + step), jnp.concatenate([p[:, :h], m[:, :h]], 1))
                    put(2 + j, slice(h + t, h + t + step), jnp.concatenate([p[:, h:], m[:, h:]], 1))

        def mul_d():
            Y[2] = left(2, 2)
            Y[3] = left(6, 3)

        def store():
            for t in range(0, h, step):
                for sign, base in ((1, t), (-1, h + t)):
                    rows = slice(base, base + step)
                    if sign == 1:
                        hr = Y[2, t:t + step, :] + Y[3, t:t + step, :]
                        hi = Y[2, h + t:h + t + step, :] + Y[3, h + t:h + t + step, :]
                    else:
                        hr = Y[2, t:t + step, :] - Y[3, t:t + step, :]
                        hi = Y[2, h + t:h + t + step, :] - Y[3, h + t:h + t + step, :]
                    p0, p1 = PR[s, 0, rows, :], PR[s, 1, rows, :]
                    scatter(0, base, p0 * hr + p1 * hi)
                    scatter(1, base, p0 * hi - p1 * hr)

        return [load, mul_a, mix_b, mul_b, mix_c, mul_c, mix_d, mul_d, store]

    ti = lax.broadcasted_iota(jnp.int32, (8, 128), 0)

    def lanes(acc):
        total = acc[:, 0:128]
        for q in range(128, acc.shape[1], 128):
            total = total + acc[:, q:q + 128]
        return jnp.sum(total, axis=0, keepdims=True)

    def iteration(it, carry):
        alpha_before, rr_before = carry
        last = it + 1 == ITERS

        def norm(i, acc):
            v = R[:, pl.ds(pl.multiple_of(h + i * 32, 32), 32), own]
            return acc + fold(v[0] * v[0]) + fold(v[1] * v[1])
        rr_acc = lax.fori_loop(0, side // 32, norm, jnp.zeros((8, side), F32))

        order = [*range(2, cap), 0, 1]
        seen = set()
        acc = [jnp.zeros((8, side), F32)]
        timed = []
        for n, s in enumerate(order):
            for q, stage in enumerate(patch(s, n % 2, seen, acc)):
                timed.append((SKEW * n + q, n, stage))
        for _, _, stage in sorted(timed, key=lambda x: x[:2]):
            stage()
        acc = acc[0]

        re_edge = [
            both(q, S.at[0, top_h, e], RA.at[0, :, e], S.at[0, end_h, e], RA.at[1, :, e], 0)
            for q, e in enumerate(edges)
        ]
        im_edge = [
            both(2 + q, S.at[1, e, top_h], CC.at[0, e, :], S.at[1, e, end_h], CC.at[1, e, :], 1)
            for q, e in enumerate(edges)
        ]
        re_mid = both(4, S.at[0, top_h, own], RA.at[0, :, own], S.at[0, end_h, own], RA.at[1, :, own], 0)
        im_mid = both(5, S.at[1, own, top_h], CC.at[0, own, :], S.at[1, own, end_h], CC.at[1, own, :], 1)
        for start, _ in (*re_edge, *im_edge, re_mid, im_mid):
            start()
        rr_l, pap_l = lanes(rr_acc), lanes(acc)
        T1[it, row] = jnp.where(ti == 0, rr_l, jnp.where(ti == 1, pap_l + RIDGE * rr_l, 0.0))
        ones = [
            pltpu.make_async_remote_copy(
                src_ref=T1.at[it, row], dst_ref=T1.at[it, row], send_sem=s1_send.at[it, d],
                recv_sem=s1_recv.at[it, d], device_id=(lax.rem(row + d, n_row), col), device_id_type=MESH)
            for d in range(1, n_row)
        ]
        for copy in ones:
            copy.start()
        for _, done in re_edge:
            done()

        def add_rows(i, carry):
            near = pl.ds(pl.multiple_of(i * 32, 32), 32)
            for q in range(2):
                rows = pl.ds(pl.multiple_of((1 + q) * h + i * 32, 32), 32)
                for e in edges:
                    S[0, rows, e] += RA[1 - q, near, e]
            return carry
        lax.fori_loop(0, h // 32, add_rows, 0)
        re_turn = both(6, S.at[0, own, top_h], CA.at[0], S.at[0, own, end_h], CA.at[1], 1)
        re_turn[0]()
        for _, done in im_edge:
            done()

        def add_cols(i, carry):
            for base in (0, 3 * h):
                rows = pl.ds(pl.multiple_of(base + i * 32, 32), 32)
                S[1, rows, one] += CC[1, rows, :]
                S[1, rows, two] += CC[0, rows, :]
            return carry
        lax.fori_loop(0, h // 32, add_cols, 0)
        im_turn = both(7, S.at[1, top_h, own], RC.at[0], S.at[1, end_h, own], RC.at[1], 0)
        im_turn[0]()
        for copy in ones:
            copy.wait()
        total = T1[it, 0]
        for q in range(1, n_row):
            total = total + T1[it, q]
        T2[it, col] = total
        twos = [
            pltpu.make_async_remote_copy(
                src_ref=T2.at[it, col], dst_ref=T2.at[it, col], send_sem=s2_send.at[it, d],
                recv_sem=s2_recv.at[it, d], device_id=(row, lax.rem(col + d, n_col)), device_id_type=MESH)
            for d in range(1, n_col)
        ]
        for copy in twos:
            copy.start()
        re_mid[1]()
        im_mid[1]()
        re_turn[1]()
        im_turn[1]()

        def make(i, carry):
            near = pl.ds(pl.multiple_of(i * 32, 32), 32)
            for q in range(2):
                rows = pl.ds(pl.multiple_of((1 + q) * h + i * 32, 32), 32)
                inner = pl.ds(pl.multiple_of(q * h + i * 32, 32), 32)
                re = S[0, rows, own] + RA[1 - q, near, own]
                im = S[1, rows, own] + RC[1 - q, near, :]
                G[0, rows, one] = re[:, :h] + CA[1, inner, :]
                G[0, rows, two] = re[:, h:] + CA[0, inner, :]
                G[1, rows, one] = im[:, :h] + CC[1, rows, :]
                G[1, rows, two] = im[:, h:] + CC[0, rows, :]
            return carry
        lax.fori_loop(0, h // 32, make, 0)

        def scalars():
            for copy in twos:
                copy.wait()
            total = T2[it, 0]
            for q in range(1, n_col):
                total = total + T2[it, q]
            rr = jnp.sum(jnp.where(ti == 0, total, 0.0), keepdims=True)
            pap = jnp.sum(jnp.where(ti == 1, total, 0.0), keepdims=True)
            ratio = jnp.where(it == 0, 0.0, rr / rr_before)
            return rr, ratio, rr / (pap - ratio * rr / alpha_before)

        @pl.when(jnp.logical_not(last))
        def _():
            wait = gather(G)
            wait()

        rr, ratio, alpha = scalars()

        def advance(i, carry):
            near = pl.ds(pl.multiple_of(i * 32, 32), 32)
            rows = pl.ds(pl.multiple_of(h + i * 32, 32), 32)
            for c in range(2):
                d = R[c, rows, own] + ratio * D[c, near, :]
                D[c, near, :] = d
                SOL[c, near, :] += alpha * d
            return carry
        lax.fori_loop(0, side // 32, advance, 0)

        def advance_r(rows):
            for c in range(2):
                r = R[c, rows, :]
                along = G[c, rows, :] + RIDGE * r + ratio * L[c, rows, :]
                L[c, rows, :] = along
                R[c, rows, :] = r - alpha * along
        chunks(2 * side, 32, advance_r)
        return alpha, rr

    one11 = jnp.ones((1, 1), F32)
    lax.fori_loop(0, ITERS, iteration, (one11, one11))

    def emit(rows):
        res_ref[:, rows, :] = R[:, pl.ds(pl.multiple_of(rows.start + h, 32), 32), own]
    chunks(side, 32, emit)


def solution(mesh):
    n_row, n_col = mesh.shape["row"], mesh.shape["col"]

    def local(right_side, probe, weights, offsets, counts):
        side = probe.shape[1]
        cap = offsets.shape[2]
        h = side // 2
        mats = jnp.asarray(tables(side))
        block = jax.ShapeDtypeStruct((2, side, side), F32)
        hbm = pl.BlockSpec(memory_space=pltpu.HBM)
        smem = pl.BlockSpec(memory_space=pltpu.SMEM)
        wide = pltpu.VMEM((2, 2 * side, 2 * side), F32)
        tile = pltpu.VMEM((2, side, side), F32)
        dma = pltpu.SemaphoreType.DMA
        vmem = pl.BlockSpec(memory_space=pltpu.VMEM)
        return pl.pallas_call(
            functools.partial(kernel, n_row, n_col, cap, side),
            out_shape=(block, block),
            in_specs=[smem, smem, hbm, hbm, hbm, hbm],
            out_specs=(vmem, vmem),
            scratch_shapes=[
                wide, wide, wide, wide,
                tile,
                pltpu.VMEM((cap, 2, side, side), F32),
                tile,
                pltpu.VMEM((side, side), F32),
                pltpu.VMEM((8, side, side), BF16),
                pltpu.VMEM((4, 2, side, side), BF16),
                pltpu.VMEM((4, 2, side, side), BF16),
                pltpu.VMEM((4, side, side), F32),
                pltpu.VMEM((4, side, side), F32),
                tile,
                pltpu.VMEM((2, h, 2 * side), F32),
                pltpu.VMEM((2, side, h), F32),
                pltpu.VMEM((2, 2 * side, h), F32),
                pltpu.VMEM((2, h, side), F32),
                pltpu.VMEM((ITERS, n_row, 8, 128), F32),
                pltpu.VMEM((ITERS, n_col, 8, 128), F32),
                dma((32,)), dma((32,)),
                dma((ITERS, n_row)), dma((ITERS, n_row)),
                dma((ITERS, n_col)), dma((ITERS, n_col)),
                dma((4,)),
            ],
            compiler_params=pltpu.CompilerParams(
                collective_id=0, has_side_effects=True, vmem_limit_bytes=53824 * 1024),
        )(offsets[0, 0].T, counts, right_side, probe, weights, mats)

    placed = (P(None, "row", "col"), P(), P(), P("row", "col", None, None), P("row", "col"))
    return jax.shard_map(
        local, mesh=mesh, in_specs=placed, out_specs=(P(None, "row", "col"), P(None, "row", "col")), check_vma=False)
```

```python
import functools
import math

import jax
import jax.numpy as jnp
import numpy as np
from jax import lax
from jax.experimental import pallas as pl
from jax.experimental.pallas import tpu as pltpu
from jax.sharding import PartitionSpec as P

ITERS = 3
RIDGE = 0.5
SKEW = 1.0
MESH = pl.DeviceIdType.MESH
F32 = jnp.float32
BF16 = jnp.bfloat16


def tables(length):
    half = length // 2
    k = np.arange(half)[:, None]
    n = np.arange(half)[None, :]
    out = []
    for odd in (0, 1):
        angle = 2.0 * math.pi * ((n * (2 * k + odd)) % length) / length
        re, im = np.cos(angle) / math.sqrt(length), -np.sin(angle) / math.sqrt(length)
        real = np.block([[re, -im], [im, re]])
        for mat in (real, real.T):
            hi = mat.astype(BF16)
            out += [hi, (mat - hi.astype(np.float64)).astype(BF16)]
    return np.stack(out)


def kernel(
    n_row, n_col, n_x, cap, side,
    off_ref, cnt_ref, rhs_hbm, probe_hbm, w_hbm, mat_hbm,
    SOL, res_ref,
    R, G, L, S, D, PR, P0, W0, mat_ref, XS, YS, W, RXI, RXO, DXI, DXO, ZR, DZ, T1, T2,
    one_send, one_recv, two_send, two_recv, s1_send, s1_recv, s2_send, s2_recv, io_sem,
):
    h = side // 2
    own = slice(h, h + side)
    row = lax.axis_index("row")
    col = lax.axis_index("col")

    load_r = pltpu.make_async_copy(rhs_hbm, R.at[:, own, own], io_sem.at[0])
    load_p = pltpu.make_async_copy(probe_hbm, P0, io_sem.at[1])
    load_w = pltpu.make_async_copy(w_hbm, W0, io_sem.at[2])
    load_m = pltpu.make_async_copy(mat_hbm, mat_ref, io_sem.at[3])
    for load in (load_r, load_p, load_w, load_m):
        load.start()

    def chunks(total, step, body):
        def run(i, carry):
            body(pl.multiple_of(i * step, step))
            return carry
        lax.fori_loop(0, total // step, run, 0)

    def fill(buf, rows, cols):
        def run(at):
            buf[:, pl.ds(pl.multiple_of(rows.start + at, 32), 32), cols] = jnp.zeros(
                (2, 32, cols.stop - cols.start), F32)
        chunks(rows.stop - rows.start, 32, run)

    every = slice(0, 2 * side)
    one, two, top_h, end_h = slice(h, 2 * h), slice(2 * h, 3 * h), slice(0, h), slice(3 * h, 4 * h)
    lefts, rights = slice(0, side), slice(side, 2 * side)
    left_ok, right_ok = col > 0, col < n_col - 1
    pl.when(row == 0)(lambda: fill(R, top_h, every))
    pl.when(row == n_row - 1)(lambda: fill(R, end_h, every))
    pl.when(col == 0)(lambda: fill(R, every, top_h))
    pl.when(col == n_col - 1)(lambda: fill(R, every, end_h))

    barrier = pltpu.get_barrier_semaphore()
    for d in range(1, n_row):
        pl.semaphore_signal(barrier, inc=1, device_id=(lax.rem(row + d, n_row), col), device_id_type=MESH)
    for d in range(1, n_col):
        pl.semaphore_signal(barrier, inc=1, device_id=(row, lax.rem(col + d, n_col)), device_id_type=MESH)
    pl.semaphore_wait(barrier, n_row - 1 + n_col - 1)

    odd = lax.rem(row, 2)
    inner_row = row + 1 - 2 * odd
    outer_row = row - 1 + 2 * odd
    inner_ok = inner_row < n_row
    outer_ok = jnp.logical_and(outer_row >= 0, outer_row < n_row)
    bent = lax.rem((row + 1) // 2, n_x) == 0
    z_first = (jnp.logical_and(bent, outer_ok), outer_ok)
    x_first = tuple(jnp.logical_not(z) for z in z_first)
    x_pair = tuple(jnp.logical_and(x, outer_ok) for x in x_first)

    def band(start, size=h):
        return pl.ds(pl.multiple_of(start, h), size)

    inn, inn_halo, inn_there = band((2 - odd) * h), band(3 * h * (1 - odd)), band(3 * h * odd)
    out, out_halo, out_there = band((1 + odd) * h), band(3 * h * odd), band(3 * h * (1 - odd))
    outer = band(2 * h * odd, side)

    class Swap:
        def __init__(self, sems, parts):
            send, recv = sems
            self.parts = []
            for q, (src, dst, device, sends, gets) in enumerate(parts):
                self.parts.append((pltpu.make_async_remote_copy(
                    src_ref=src, dst_ref=dst, send_sem=send(q), recv_sem=recv(q),
                    device_id=device, device_id_type=MESH), sends, gets))

        def start(self):
            for copy, sends, _ in self.parts:
                pl.when(sends)(copy.start)

        def wait(self):
            for copy, sends, gets in self.parts:
                pl.when(sends)(copy.wait_send)
                pl.when(gets)(copy.wait_recv)

    def once(index):
        return (lambda q: one_send.at[index + q]), (lambda q: one_recv.at[index + q])

    def turn(index, phase):
        return (lambda q: two_send.at[phase, index + q]), (lambda q: two_recv.at[phase, index + q])

    def across(sems, left_src, left_dst, right_src, right_dst, on):
        go_left, go_right = jnp.logical_and(on, left_ok), jnp.logical_and(on, right_ok)
        return Swap(sems, [
            (left_src, left_dst, (row, col - 1), go_left, go_right),
            (right_src, right_dst, (row, col + 1), go_right, go_left)])

    def along(sems, src, dst, there, on):
        return Swap(sems, [(src, dst, (there, col), on, on)])

    yes = col >= 0

    def spread(F):
        ends = [
            across(once(20 + 2 * c), F.at[c, out, one], F.at[c, out, end_h], F.at[c, out, two], F.at[c, out, top_h], yes)
            for c in range(2)
        ]
        mids = across(once(24), F.at[:, inn, one], F.at[:, inn, end_h], F.at[:, inn, two], F.at[:, inn, top_h], yes)
        firsts = [along(once(26 + c), F.at[c, out, own], F.at[c, out_there, own], outer_row, z_first[c]) for c in range(2)]
        ends[0].start()
        firsts[1].start()
        firsts[0].start()
        mids.start()
        ends[1].start()
        laters = []
        ends[0].wait()
        laters.append(along(once(28), F.at[0, out, :], F.at[0, out_there, :], outer_row, x_pair[0]))
        laters[-1].start()
        for c in (1, 0):
            firsts[c].wait()
            laters.append(across(
                once(30 + 2 * c), F.at[c, out_halo, one], F.at[c, out_halo, end_h],
                F.at[c, out_halo, two], F.at[c, out_halo, top_h], z_first[c]))
            laters[-1].start()
        mids.wait()
        laters.append(along(once(34), F.at[:, inn, :], F.at[:, inn_there, :], inner_row, inner_ok))
        laters[-1].start()
        ends[1].wait()
        laters.append(along(once(29), F.at[1, out, :], F.at[1, out_there, :], outer_row, x_pair[1]))
        laters[-1].start()

        def wait():
            for swap in laters:
                swap.wait()

        return wait

    load_r.wait()
    spread_wait = spread(R)

    fill(G, every, every)
    fill(L, every, every)
    for buf in (D, SOL):
        fill(buf, slice(0, buf.shape[1]), slice(0, buf.shape[2]))

    load_p.wait()
    for s in range(cap):
        on = jnp.where(s < cnt_ref[0, 0], 1.0, 0.0).astype(F32)
        for c in range(2):
            rolled = pltpu.roll(P0[c], off_ref[0, s] + h, 0)
            PR[s, c] = pltpu.roll(rolled, off_ref[1, s] + h, 1) * on

    def three(val):
        top = val.astype(BF16)
        rest = val - top.astype(F32)
        mid = rest.astype(BF16)
        return top, mid, (rest - mid.astype(F32)).astype(BF16)

    load_w.wait()
    first = lax.broadcasted_iota(jnp.int32, (side, side), 0)
    second = lax.broadcasted_iota(jnp.int32, (side, side), 1)
    freq = jnp.where(first >= h, 2 * (first - h) + 1, 2 * first)
    pick = jnp.where(second == freq, 1.0, 0.0).astype(BF16)
    by_row = sum(jnp.dot(pick, part, preferred_element_type=F32) for part in three(W0[...]))
    parts = three(by_row)
    lane = jnp.where(second >= h, second - h, second)
    for q in range(2):
        pick = jnp.where(first == 2 * lane + q, 1.0, 0.0).astype(BF16)
        W[q] = sum(jnp.dot(part, pick, preferred_element_type=F32) for part in parts)

    load_m.wait()
    spread_wait()

    step = 32

    def fold(val):
        return jnp.sum(val.reshape(-1, 8, val.shape[-1]), axis=0)

    sub = lax.broadcasted_iota(jnp.int32, (step, h), 0)
    lan = lax.broadcasted_iota(jnp.int32, (step, h), 1)

    def side_of(s, at):
        if s == 0:
            return "both" if at < h else "near"
        if s == 1:
            return "far" if at < h else "both"
        return "both"

    def patch(s, k, seen, acc):
        X, Y = XS[k], YS[k]
        a = off_ref[0, s] + h
        b = off_ref[1, s] + h

        def put(j, rows, val):
            hi = val.astype(BF16)
            X[j, 0, rows, :] = hi
            X[j, 1, rows, :] = (val - hi.astype(F32)).astype(BF16)

        def left(m, j):
            hi, lo = mat_ref[m], mat_ref[m + 1]
            xh, xl = X[j, 0], X[j, 1]
            return jnp.dot(
                jnp.concatenate([hi, lo, hi], 1), jnp.concatenate([xh, xh, xl], 0), preferred_element_type=F32)

        def right(j, m):
            hi, lo = mat_ref[m], mat_ref[m + 1]
            xh, xl = X[j, 0], X[j, 1]
            return jnp.dot(
                jnp.concatenate([xh, xl, xh], 1), jnp.concatenate([hi, hi, lo], 0), preferred_element_type=F32)

        def covered(c, base):
            halves = []
            for at in (0, h):
                cols, fcols = slice(at, at + h), slice(side + at, side + at + h)
                rk, ck = side_of(s, base), side_of(s, at)
                rows, far = slice(base, base + step), slice(side + base, side + base + step)

                def in_cols(r):
                    if ck == "near":
                        return R[c, r, cols]
                    if ck == "far":
                        return R[c, r, fcols]
                    return jnp.where(lan + at >= b, R[c, r, cols], R[c, r, fcols])

                if rk == "near":
                    halves.append(in_cols(rows))
                elif rk == "far":
                    halves.append(in_cols(far))
                else:
                    halves.append(jnp.where(sub + base >= a, in_cols(rows), in_cols(far)))
            return jnp.concatenate(halves, 1)

        def scatter(c, base, term):
            for at in (0, h):
                val = term[:, at:at + h]
                rk, ck = side_of(s, base), side_of(s, at)
                rows = {}
                if rk == "both":
                    near = jnp.where(sub + base >= a, val, 0.0)
                    rows = {0: near, side: val - near}
                else:
                    rows = {0 if rk == "near" else side: val}
                for shift, part in rows.items():
                    if ck == "both":
                        near = jnp.where(lan + at >= b, part, 0.0)
                        cells = {0: near, side: part - near}
                    else:
                        cells = {0 if ck == "near" else side: part}
                    for over, cell in cells.items():
                        r0, c0 = shift + base, over + at
                        where = (c, slice(r0, r0 + step), slice(c0, c0 + h))
                        if (c, r0, c0) in seen:
                            S[where] += cell
                        else:
                            S[where] = cell
                            seen.add((c, r0, c0))

        def load():
            for t in range(0, h, step):
                parts = []
                for base in (t, h + t):
                    rows = slice(base, base + step)
                    v = [covered(c, base) for c in range(2)]
                    p0, p1 = PR[s, 0, rows, :], PR[s, 1, rows, :]
                    parts.append((p0 * v[0] - p1 * v[1], p0 * v[1] + p1 * v[0]))
                for c in range(2):
                    rows = slice(c * h + t, c * h + t + step)
                    put(0, rows, parts[0][c] + parts[1][c])
                    put(1, rows, parts[0][c] - parts[1][c])

        def mul_a():
            Y[0] = left(0, 0)
            Y[1] = left(4, 1)

        def mix_b():
            for j in range(2):
                for t in range(0, h, step):
                    re, im = Y[j, t:t + step, :], Y[j, h + t:h + t + step, :]
                    rows = slice(j * h + t, j * h + t + step)
                    put(2, rows, jnp.concatenate([re[:, :h] + re[:, h:], im[:, :h] + im[:, h:]], 1))
                    put(3, rows, jnp.concatenate([re[:, :h] - re[:, h:], im[:, :h] - im[:, h:]], 1))

        def mul_b():
            Y[2] = right(2, 2)
            Y[3] = right(3, 6)

        def mix_c():
            for j in range(2):
                for t in range(0, side, step):
                    rows = slice(t, t + step)
                    f = Y[2 + j, rows, :]
                    wf = W[j, rows, :] * f
                    acc[0] = acc[0] + fold(wf * f)
                    put(j, rows, wf)

        def mul_c():
            Y[0] = right(0, 0)
            Y[1] = right(1, 4)

        def mix_d():
            for j in range(2):
                for t in range(0, h, step):
                    rows = slice(j * h + t, j * h + t + step)
                    c, d = Y[0, rows, :], Y[1, rows, :]
                    p, m = c + d, c - d
                    put(2 + j, slice(t, t + step), jnp.concatenate([p[:, :h], m[:, :h]], 1))
                    put(2 + j, slice(h + t, h + t + step), jnp.concatenate([p[:, h:], m[:, h:]], 1))

        def mul_d():
            Y[2] = left(2, 2)
            Y[3] = left(6, 3)

        def store():
            for t in range(0, h, step):
                for sign, base in ((1, t), (-1, h + t)):
                    rows = slice(base, base + step)
                    if sign == 1:
                        hr = Y[2, t:t + step, :] + Y[3, t:t + step, :]
                        hi = Y[2, h + t:h + t + step, :] + Y[3, h + t:h + t + step, :]
                    else:
                        hr = Y[2, t:t + step, :] - Y[3, t:t + step, :]
                        hi = Y[2, h + t:h + t + step, :] - Y[3, h + t:h + t + step, :]
                    p0, p1 = PR[s, 0, rows, :], PR[s, 1, rows, :]
                    scatter(0, base, p0 * hr + p1 * hi)
                    scatter(1, base, p0 * hi - p1 * hr)

        return [load, mul_a, mix_b, mul_b, mix_c, mul_c, mix_d, mul_d, store]

    ti = lax.broadcasted_iota(jnp.int32, (8, 128), 0)

    def lanes(acc):
        total = acc[:, 0:128]
        for q in range(128, acc.shape[1], 128):
            total = total + acc[:, q:q + 128]
        return jnp.sum(total, axis=0, keepdims=True)

    def iteration(it, carry):
        alpha_before, rr_before = carry
        last = it + 1 == ITERS

        def norm(i, acc):
            v = R[:, pl.ds(pl.multiple_of(h + i * 32, 32), 32), own]
            return acc + fold(v[0] * v[0]) + fold(v[1] * v[1])
        rr_acc = lax.fori_loop(0, side // 32, norm, jnp.zeros((8, side), F32))

        order = [*range(2, cap), 0, 1]
        seen = set()
        acc = [jnp.zeros((8, side), F32)]
        timed = []
        for n, s in enumerate(order):
            for q, stage in enumerate(patch(s, n, seen, acc)):
                timed.append((SKEW * n + q, n, stage))
        for _, _, stage in sorted(timed, key=lambda x: x[:2]):
            stage()
        acc = acc[0]

        phase = lax.rem(it, 2)
        rr_l, pap_l = lanes(rr_acc), lanes(acc)
        T1[it, row] = jnp.where(ti == 0, rr_l, jnp.where(ti == 1, pap_l + RIDGE * rr_l, 0.0))
        ones = [
            pltpu.make_async_remote_copy(
                src_ref=T1.at[it, row], dst_ref=T1.at[it, row], send_sem=s1_send.at[it, d],
                recv_sem=s1_recv.at[it, d], device_id=(lax.rem(row + d, n_row), col), device_id_type=MESH)
            for d in range(1, n_row)
        ]
        for copy in ones:
            copy.start()

        fold_z = [
            across(once(2 * c), S.at[c, outer, top_h], ZR.at[1, c], S.at[c, outer, end_h], ZR.at[0, c], z_first[c])
            for c in range(2)
        ]
        fold_x = [along(once(4 + c), S.at[c, out_halo, :], RXO.at[c], outer_row, x_pair[c]) for c in range(2)]
        fold_i = along(once(6), S.at[:, inn_halo, :], RXI, inner_row, inner_ok)
        for swap in (fold_z[1], fold_z[0], fold_x[0], fold_i, fold_x[1]):
            swap.start()

        more = jnp.logical_not(last)

        def meet(index, rows, buf, on):
            def pick(c0, c1):
                return S.at[:, rows, c0:c1] if buf is DXI else S.at[buf, rows, c0:c1]

            def slot(from_side, c0, c1):
                return DXI.at[phase, from_side, :, :, c0:c1] if buf is DXI else DXO.at[phase, from_side, buf, :, c0:c1]

            full = across(turn(index, phase), pick(0, side), slot(1, 0, side), pick(side, 2 * side), slot(0, 0, side),
                          jnp.logical_and(on, more))
            part = across(turn(index, phase), pick(0, h), slot(1, 0, h), pick(3 * h, 4 * h), slot(0, h, side),
                          jnp.logical_and(on, last))
            return full, part

        meet_i = meet(0, inn, DXI, yes)
        meet_x = [meet(2 + 2 * c, out, c, x_first[c]) for c in range(2)]
        meet_z = [
            (
                along(turn(6 + c, phase), S.at[c, outer, own], DZ.at[phase, c], outer_row,
                      jnp.logical_and(z_first[c], more)),
                along(turn(6 + c, phase), S.at[c, out_halo, own], DZ.at[phase, c, band(h * odd), :], outer_row,
                      jnp.logical_and(z_first[c], last)),
            )
            for c in range(2)
        ]

        def begin(pair):
            for swap in pair:
                swap.start()

        def end(pair):
            for swap in pair:
                swap.wait()

        def rows_of(ref_rows, at):
            return pl.ds(pl.multiple_of(ref_rows.start + at, 32), 32)

        fold_i.wait()

        @pl.when(inner_ok)
        def _():
            def add(at):
                S[:, rows_of(inn, at), :] += RXI[:, pl.ds(at, 32), :]
            chunks(h, 32, add)
        begin(meet_i)
        for c in (1, 0):
            fold_z[c].wait()
            for ok, cols, q in ((left_ok, one, 0), (right_ok, two, 1)):
                @pl.when(jnp.logical_and(z_first[c], ok))
                def _(c=c, cols=cols, q=q):
                    def add(at):
                        S[c, rows_of(outer, at), cols] += ZR[q, c, pl.ds(at, 32), :]
                    chunks(side, 32, add)
            begin(meet_z[c])
        for c in range(2):
            fold_x[c].wait()

            @pl.when(x_pair[c])
            def _(c=c):
                def add(at):
                    S[c, rows_of(out, at), :] += RXO[c, pl.ds(at, 32), :]
                chunks(h, 32, add)
            begin(meet_x[c])

        for copy in ones:
            copy.wait()
        total = T1[it, 0]
        for q in range(1, n_row):
            total = total + T1[it, q]
        T2[it, col] = total
        twos = [
            pltpu.make_async_remote_copy(
                src_ref=T2.at[it, col], dst_ref=T2.at[it, col], send_sem=s2_send.at[it, d],
                recv_sem=s2_recv.at[it, d], device_id=(row, lax.rem(col + d, n_col)), device_id_type=MESH)
            for d in range(1, n_col)
        ]
        for copy in twos:
            copy.start()

        def settle(c, rows, got):
            def run(at):
                here, there = rows_of(rows, at), pl.ds(at, 32)

                @pl.when(left_ok)
                def _():
                    G[c, here, lefts] = S[c, here, lefts] + got(0, there)

                @pl.when(right_ok)
                def _():
                    G[c, here, rights] = S[c, here, rights] + got(1, there)

                @pl.when(jnp.logical_not(left_ok))
                def _():
                    G[c, here, one] = S[c, here, one]

                @pl.when(jnp.logical_not(right_ok))
                def _():
                    G[c, here, two] = S[c, here, two]
            chunks(h, 32, run)

        share_i = along(once(8), G.at[:, inn, :], G.at[:, inn_there, :], inner_row, jnp.logical_and(inner_ok, more))
        share_x = [
            along(once(10 + c), G.at[c, out, :], G.at[c, out_there, :], outer_row, jnp.logical_and(x_pair[c], more))
            for c in range(2)
        ]
        share_z = [
            across(once(12 + 2 * c), G.at[c, outer, one], G.at[c, outer, end_h], G.at[c, outer, two],
                   G.at[c, outer, top_h], jnp.logical_and(z_first[c], more))
            for c in range(2)
        ]
        end(meet_i)
        for c in range(2):
            settle(c, inn, lambda q, there, c=c: DXI[phase, q, c, there, :])
        share_i.start()
        for c in range(2):
            end(meet_x[c])

            @pl.when(x_first[c])
            def _(c=c):
                settle(c, out, lambda q, there: DXO[phase, q, c, there, :])
            share_x[c].start()
        for c in (1, 0):
            end(meet_z[c])

            @pl.when(z_first[c])
            def _(c=c):
                def run(at):
                    here = rows_of(outer, at)
                    G[c, here, own] = S[c, here, own] + DZ[phase, c, pl.ds(at, 32), :]
                chunks(side, 32, run)
            share_z[c].start()

        for copy in twos:
            copy.wait()
        total = T2[it, 0]
        for q in range(1, n_col):
            total = total + T2[it, q]
        rr = jnp.sum(jnp.where(ti == 0, total, 0.0), keepdims=True)
        pap = jnp.sum(jnp.where(ti == 1, total, 0.0), keepdims=True)
        ratio = jnp.where(it == 0, 0.0, rr / rr_before)
        alpha = rr / (pap - ratio * rr / alpha_before)

        def advance(i, carry):
            near = pl.ds(pl.multiple_of(i * 32, 32), 32)
            rows = pl.ds(pl.multiple_of(h + i * 32, 32), 32)
            for c in range(2):
                d = R[c, rows, own] + ratio * D[c, near, :]
                D[c, near, :] = d
                SOL[c, near, :] += alpha * d
            return carry
        lax.fori_loop(0, side // 32, advance, 0)

        for swap in (share_i, *share_x, *share_z):
            swap.wait()

        @pl.when(more)
        def _():
            def advance_r(at):
                rows = pl.ds(at, 32)
                for c in range(2):
                    r = R[c, rows, :]
                    image = G[c, rows, :] + RIDGE * r + ratio * L[c, rows, :]
                    L[c, rows, :] = image
                    R[c, rows, :] = r - alpha * image
            chunks(2 * side, 32, advance_r)

        @pl.when(last)
        def _():
            def emit(at):
                rows = pl.ds(pl.multiple_of(h + at, 32), 32)
                for c in range(2):
                    r = R[c, rows, own]
                    image = G[c, rows, own] + RIDGE * r + ratio * L[c, rows, own]
                    res_ref[c, pl.ds(at, 32), :] = r - alpha * image
            chunks(side, 32, emit)
        return alpha, rr

    one11 = jnp.ones((1, 1), F32)
    lax.fori_loop(0, ITERS, iteration, (one11, one11))


def solution(mesh):
    n_row, n_col = mesh.shape["row"], mesh.shape["col"]
    n_x = len({tuple(getattr(d, "coords", (d.id,)))[0] for d in mesh.devices.flat})

    def local(right_side, probe, weights, offsets, counts):
        side = probe.shape[1]
        cap = offsets.shape[2]
        h = side // 2
        mats = jnp.asarray(tables(side))
        block = jax.ShapeDtypeStruct((2, side, side), F32)
        hbm = pl.BlockSpec(memory_space=pltpu.HBM)
        smem = pl.BlockSpec(memory_space=pltpu.SMEM)
        wide = pltpu.VMEM((2, 2 * side, 2 * side), F32)
        tile = pltpu.VMEM((2, side, side), F32)
        dma = pltpu.SemaphoreType.DMA
        vmem = pl.BlockSpec(memory_space=pltpu.VMEM)
        return pl.pallas_call(
            functools.partial(kernel, n_row, n_col, n_x, cap, side),
            out_shape=(block, block),
            in_specs=[smem, smem, hbm, hbm, hbm, hbm],
            out_specs=(vmem, vmem),
            scratch_shapes=[
                wide, wide, wide, wide,
                tile,
                pltpu.VMEM((cap, 2, side, side), F32),
                tile,
                pltpu.VMEM((side, side), F32),
                pltpu.VMEM((8, side, side), BF16),
                [pltpu.VMEM((4, 2, side, side), BF16) for _ in range(cap)],
                [pltpu.VMEM((4, side, side), F32) for _ in range(cap)],
                tile,
                pltpu.VMEM((2, h, 2 * side), F32),
                pltpu.VMEM((2, h, 2 * side), F32),
                pltpu.VMEM((2, 2, 2, h, side), F32),
                pltpu.VMEM((2, 2, 2, h, side), F32),
                pltpu.VMEM((2, 2, side, h), F32),
                pltpu.VMEM((2, 2, side, side), F32),
                pltpu.VMEM((ITERS, n_row, 8, 128), F32),
                pltpu.VMEM((ITERS, n_col, 8, 128), F32),
                dma((36,)), dma((36,)), dma((2, 8)), dma((2, 8)),
                dma((ITERS, n_row)), dma((ITERS, n_row)),
                dma((ITERS, n_col)), dma((ITERS, n_col)),
                dma((4,)),
            ],
            compiler_params=pltpu.CompilerParams(
                collective_id=0, has_side_effects=True, vmem_limit_bytes=53824 * 1024),
        )(offsets[0, 0].T, counts, right_side, probe, weights, mats)

    placed = (P(None, "row", "col"), P(), P(), P("row", "col", None, None), P("row", "col"))
    return jax.shard_map(
        local, mesh=mesh, in_specs=placed, out_specs=(P(None, "row", "col"), P(None, "row", "col")), check_vma=False)
```

```python
import functools
import math

import jax
import jax.numpy as jnp
import numpy as np
from jax import lax
from jax.experimental import pallas as pl
from jax.experimental.pallas import tpu as pltpu
from jax.sharding import PartitionSpec as P

ITERS = 3
RIDGE = 0.5
SKEW = 1.0
MESH = pl.DeviceIdType.MESH
F32 = jnp.float32
BF16 = jnp.bfloat16


def tables(length):
    half = length // 2
    k = np.arange(half)[:, None]
    n = np.arange(half)[None, :]
    out = []
    for odd in (0, 1):
        angle = 2.0 * math.pi * ((n * (2 * k + odd)) % length) / length
        re, im = np.cos(angle) / math.sqrt(length), -np.sin(angle) / math.sqrt(length)
        real = np.block([[re, -im], [im, re]])
        for mat in (real, real.T):
            hi = mat.astype(BF16)
            out += [hi, (mat - hi.astype(np.float64)).astype(BF16)]
    return np.stack(out)


def kernel(
    n_row, n_col, n_x, cap, side,
    off_ref, cnt_ref, rhs_hbm, probe_hbm, w_hbm, mat_hbm,
    SOL, res_ref,
    R, G, L, S, D, PR, P0, W0, mat_ref, XS, YS, W, RXI, RXO, DXI, DXO, ZR, DZ, T1, T2,
    one_send, one_recv, two_send, two_recv, s1_send, s1_recv, s2_send, s2_recv, io_sem,
):
    h = side // 2
    own = slice(h, h + side)
    row = lax.axis_index("row")
    col = lax.axis_index("col")

    load_r = pltpu.make_async_copy(rhs_hbm, R.at[:, own, own], io_sem.at[0])
    load_p = pltpu.make_async_copy(probe_hbm, P0, io_sem.at[1])
    load_w = pltpu.make_async_copy(w_hbm, W0, io_sem.at[2])
    load_m = pltpu.make_async_copy(mat_hbm, mat_ref, io_sem.at[3])
    for load in (load_r, load_p, load_w, load_m):
        load.start()

    def chunks(total, step, body):
        def run(i, carry):
            body(pl.multiple_of(i * step, step))
            return carry
        lax.fori_loop(0, total // step, run, 0)

    def fill(buf, rows, cols):
        def run(at):
            buf[:, pl.ds(pl.multiple_of(rows.start + at, 32), 32), cols] = jnp.zeros(
                (2, 32, cols.stop - cols.start), F32)
        chunks(rows.stop - rows.start, 32, run)

    every = slice(0, 2 * side)
    one, two, top_h, end_h = slice(h, 2 * h), slice(2 * h, 3 * h), slice(0, h), slice(3 * h, 4 * h)
    lefts, rights = slice(0, side), slice(side, 2 * side)
    left_ok, right_ok = col > 0, col < n_col - 1
    pl.when(row == 0)(lambda: fill(R, top_h, every))
    pl.when(row == n_row - 1)(lambda: fill(R, end_h, every))
    pl.when(col == 0)(lambda: fill(R, every, top_h))
    pl.when(col == n_col - 1)(lambda: fill(R, every, end_h))

    barrier = pltpu.get_barrier_semaphore()
    for d in range(1, n_row):
        pl.semaphore_signal(barrier, inc=1, device_id=(lax.rem(row + d, n_row), col), device_id_type=MESH)
    for d in range(1, n_col):
        pl.semaphore_signal(barrier, inc=1, device_id=(row, lax.rem(col + d, n_col)), device_id_type=MESH)
    pl.semaphore_wait(barrier, n_row - 1 + n_col - 1)

    odd = lax.rem(row, 2)
    inner_row = row + 1 - 2 * odd
    outer_row = row - 1 + 2 * odd
    inner_ok = inner_row < n_row
    outer_ok = jnp.logical_and(outer_row >= 0, outer_row < n_row)
    bent = lax.rem((row + 1) // 2, n_x) == 0
    z_first = (jnp.logical_and(bent, outer_ok), outer_ok)
    x_first = tuple(jnp.logical_not(z) for z in z_first)
    x_pair = tuple(jnp.logical_and(x, outer_ok) for x in x_first)

    def band(start, size=h):
        return pl.ds(pl.multiple_of(start, h), size)

    inn, inn_halo, inn_there = band((2 - odd) * h), band(3 * h * (1 - odd)), band(3 * h * odd)
    out, out_halo, out_there = band((1 + odd) * h), band(3 * h * odd), band(3 * h * (1 - odd))
    outer = band(2 * h * odd, side)

    class Swap:
        def __init__(self, sems, parts):
            send, recv = sems
            self.parts = []
            for q, (src, dst, device, sends, gets) in enumerate(parts):
                self.parts.append((pltpu.make_async_remote_copy(
                    src_ref=src, dst_ref=dst, send_sem=send(q), recv_sem=recv(q),
                    device_id=device, device_id_type=MESH), sends, gets))

        def start(self):
            for copy, sends, _ in self.parts:
                pl.when(sends)(copy.start)

        def wait(self):
            for copy, sends, gets in self.parts:
                pl.when(sends)(copy.wait_send)
                pl.when(gets)(copy.wait_recv)

    def once(index):
        return (lambda q: one_send.at[index + q]), (lambda q: one_recv.at[index + q])

    def turn(index, phase):
        return (lambda q: two_send.at[phase, index + q]), (lambda q: two_recv.at[phase, index + q])

    def across(sems, left_src, left_dst, right_src, right_dst, on):
        go_left, go_right = jnp.logical_and(on, left_ok), jnp.logical_and(on, right_ok)
        return Swap(sems, [
            (left_src, left_dst, (row, col - 1), go_left, go_right),
            (right_src, right_dst, (row, col + 1), go_right, go_left)])

    def leftward(sems, src, dst, on):
        return Swap(sems, [(src, dst, (row, col - 1), jnp.logical_and(on, left_ok), jnp.logical_and(on, right_ok))])

    def rightward(sems, src, dst, on):
        return Swap(sems, [(src, dst, (row, col + 1), jnp.logical_and(on, right_ok), jnp.logical_and(on, left_ok))])

    def along(sems, src, dst, there, on, gets=None):
        return Swap(sems, [(src, dst, (there, col), on, on if gets is None else gets)])

    yes = col >= 0

    def spread(F):
        ends = [
            across(once(30 + 2 * c), F.at[c, out, one], F.at[c, out, end_h], F.at[c, out, two], F.at[c, out, top_h], yes)
            for c in range(2)
        ]
        mids = across(once(34), F.at[:, inn, one], F.at[:, inn, end_h], F.at[:, inn, two], F.at[:, inn, top_h], yes)
        firsts = [along(once(36 + c), F.at[c, out, own], F.at[c, out_there, own], outer_row, z_first[c]) for c in range(2)]
        ends[0].start()
        firsts[1].start()
        firsts[0].start()
        mids.start()
        ends[1].start()
        laters = []
        ends[0].wait()
        laters.append(along(once(38), F.at[0, out, :], F.at[0, out_there, :], outer_row, x_pair[0]))
        laters[-1].start()
        for c in (1, 0):
            firsts[c].wait()
            laters.append(across(
                once(40 + 2 * c), F.at[c, out_halo, one], F.at[c, out_halo, end_h],
                F.at[c, out_halo, two], F.at[c, out_halo, top_h], z_first[c]))
            laters[-1].start()
        mids.wait()
        laters.append(along(once(44), F.at[:, inn, :], F.at[:, inn_there, :], inner_row, inner_ok))
        laters[-1].start()
        ends[1].wait()
        laters.append(along(once(39), F.at[1, out, :], F.at[1, out_there, :], outer_row, x_pair[1]))
        laters[-1].start()

        def wait():
            for swap in laters:
                swap.wait()

        return wait

    load_r.wait()
    spread_wait = spread(R)

    fill(G, every, every)
    fill(L, every, every)
    for buf in (D, SOL):
        fill(buf, slice(0, buf.shape[1]), slice(0, buf.shape[2]))

    load_p.wait()
    for s in range(cap):
        on = jnp.where(s < cnt_ref[0, 0], 1.0, 0.0).astype(F32)
        for c in range(2):
            rolled = pltpu.roll(P0[c], off_ref[0, s] + h, 0)
            PR[s, c] = pltpu.roll(rolled, off_ref[1, s] + h, 1) * on

    def three(val):
        top = val.astype(BF16)
        rest = val - top.astype(F32)
        mid = rest.astype(BF16)
        return top, mid, (rest - mid.astype(F32)).astype(BF16)

    load_w.wait()
    first = lax.broadcasted_iota(jnp.int32, (side, side), 0)
    second = lax.broadcasted_iota(jnp.int32, (side, side), 1)
    freq = jnp.where(first >= h, 2 * (first - h) + 1, 2 * first)
    pick = jnp.where(second == freq, 1.0, 0.0).astype(BF16)
    by_row = sum(jnp.dot(pick, part, preferred_element_type=F32) for part in three(W0[...]))
    parts = three(by_row)
    lane = jnp.where(second >= h, second - h, second)
    for q in range(2):
        pick = jnp.where(first == 2 * lane + q, 1.0, 0.0).astype(BF16)
        W[q] = sum(jnp.dot(part, pick, preferred_element_type=F32) for part in parts)

    load_m.wait()
    spread_wait()

    step = 32

    def fold(val):
        return jnp.sum(val.reshape(-1, 8, val.shape[-1]), axis=0)

    sub = lax.broadcasted_iota(jnp.int32, (step, h), 0)
    lan = lax.broadcasted_iota(jnp.int32, (step, h), 1)

    def side_of(s, at):
        if s == 0:
            return "both" if at < h else "near"
        if s == 1:
            return "far" if at < h else "both"
        return "both"

    def patch(s, k, seen, acc):
        X, Y = XS[k], YS[k]
        a = off_ref[0, s] + h
        b = off_ref[1, s] + h

        def put(j, rows, val):
            hi = val.astype(BF16)
            X[j, 0, rows, :] = hi
            X[j, 1, rows, :] = (val - hi.astype(F32)).astype(BF16)

        def left(m, j):
            hi, lo = mat_ref[m], mat_ref[m + 1]
            xh, xl = X[j, 0], X[j, 1]
            return jnp.dot(
                jnp.concatenate([hi, lo, hi], 1), jnp.concatenate([xh, xh, xl], 0), preferred_element_type=F32)

        def right(j, m):
            hi, lo = mat_ref[m], mat_ref[m + 1]
            xh, xl = X[j, 0], X[j, 1]
            return jnp.dot(
                jnp.concatenate([xh, xl, xh], 1), jnp.concatenate([hi, hi, lo], 0), preferred_element_type=F32)

        def covered(c, base):
            halves = []
            for at in (0, h):
                cols, fcols = slice(at, at + h), slice(side + at, side + at + h)
                rk, ck = side_of(s, base), side_of(s, at)
                rows, far = slice(base, base + step), slice(side + base, side + base + step)

                def in_cols(r):
                    if ck == "near":
                        return R[c, r, cols]
                    if ck == "far":
                        return R[c, r, fcols]
                    return jnp.where(lan + at >= b, R[c, r, cols], R[c, r, fcols])

                if rk == "near":
                    halves.append(in_cols(rows))
                elif rk == "far":
                    halves.append(in_cols(far))
                else:
                    halves.append(jnp.where(sub + base >= a, in_cols(rows), in_cols(far)))
            return jnp.concatenate(halves, 1)

        def scatter(c, base, term):
            for at in (0, h):
                val = term[:, at:at + h]
                rk, ck = side_of(s, base), side_of(s, at)
                rows = {}
                if rk == "both":
                    near = jnp.where(sub + base >= a, val, 0.0)
                    rows = {0: near, side: val - near}
                else:
                    rows = {0 if rk == "near" else side: val}
                for shift, part in rows.items():
                    if ck == "both":
                        near = jnp.where(lan + at >= b, part, 0.0)
                        cells = {0: near, side: part - near}
                    else:
                        cells = {0 if ck == "near" else side: part}
                    for over, cell in cells.items():
                        r0, c0 = shift + base, over + at
                        where = (c, slice(r0, r0 + step), slice(c0, c0 + h))
                        if (c, r0, c0) in seen:
                            S[where] += cell
                        else:
                            S[where] = cell
                            seen.add((c, r0, c0))

        def load():
            for t in range(0, h, step):
                parts = []
                for base in (t, h + t):
                    rows = slice(base, base + step)
                    v = [covered(c, base) for c in range(2)]
                    p0, p1 = PR[s, 0, rows, :], PR[s, 1, rows, :]
                    parts.append((p0 * v[0] - p1 * v[1], p0 * v[1] + p1 * v[0]))
                for c in range(2):
                    rows = slice(c * h + t, c * h + t + step)
                    put(0, rows, parts[0][c] + parts[1][c])
                    put(1, rows, parts[0][c] - parts[1][c])

        def mul_a():
            Y[0] = left(0, 0)
            Y[1] = left(4, 1)

        def mix_b():
            for j in range(2):
                for t in range(0, h, step):
                    re, im = Y[j, t:t + step, :], Y[j, h + t:h + t + step, :]
                    rows = slice(j * h + t, j * h + t + step)
                    put(2, rows, jnp.concatenate([re[:, :h] + re[:, h:], im[:, :h] + im[:, h:]], 1))
                    put(3, rows, jnp.concatenate([re[:, :h] - re[:, h:], im[:, :h] - im[:, h:]], 1))

        def mul_b():
            Y[2] = right(2, 2)
            Y[3] = right(3, 6)

        def mix_c():
            for j in range(2):
                for t in range(0, side, step):
                    rows = slice(t, t + step)
                    f = Y[2 + j, rows, :]
                    wf = W[j, rows, :] * f
                    acc[0] = acc[0] + fold(wf * f)
                    put(j, rows, wf)

        def mul_c():
            Y[0] = right(0, 0)
            Y[1] = right(1, 4)

        def mix_d():
            for j in range(2):
                for t in range(0, h, step):
                    rows = slice(j * h + t, j * h + t + step)
                    c, d = Y[0, rows, :], Y[1, rows, :]
                    p, m = c + d, c - d
                    put(2 + j, slice(t, t + step), jnp.concatenate([p[:, :h], m[:, :h]], 1))
                    put(2 + j, slice(h + t, h + t + step), jnp.concatenate([p[:, h:], m[:, h:]], 1))

        def mul_d():
            Y[2] = left(2, 2)
            Y[3] = left(6, 3)

        def store():
            for t in range(0, h, step):
                for sign, base in ((1, t), (-1, h + t)):
                    rows = slice(base, base + step)
                    if sign == 1:
                        hr = Y[2, t:t + step, :] + Y[3, t:t + step, :]
                        hi = Y[2, h + t:h + t + step, :] + Y[3, h + t:h + t + step, :]
                    else:
                        hr = Y[2, t:t + step, :] - Y[3, t:t + step, :]
                        hi = Y[2, h + t:h + t + step, :] - Y[3, h + t:h + t + step, :]
                    p0, p1 = PR[s, 0, rows, :], PR[s, 1, rows, :]
                    scatter(0, base, p0 * hr + p1 * hi)
                    scatter(1, base, p0 * hi - p1 * hr)

        return [load, mul_a, mix_b, mul_b, mix_c, mul_c, mix_d, mul_d, store]

    def lanes(acc):
        total = acc[:, 0:128]
        for q in range(128, acc.shape[1], 128):
            total = total + acc[:, q:q + 128]
        return jnp.sum(total, axis=0, keepdims=True)

    def iteration(it, carry):
        alpha_before, rr_before = carry
        last = it + 1 == ITERS

        def norm(i, acc):
            v = R[:, pl.ds(pl.multiple_of(h + i * 32, 32), 32), own]
            return acc + fold(v[0] * v[0]) + fold(v[1] * v[1])
        rr_acc = lax.fori_loop(0, side // 32, norm, jnp.zeros((8, side), F32))

        order = [*range(2, cap), 0, 1]
        seen = set()
        acc = [jnp.zeros((8, side), F32)]
        timed = []
        for n, s in enumerate(order):
            for q, stage in enumerate(patch(s, n, seen, acc)):
                timed.append((SKEW * n + q, n, stage))
        for _, _, stage in sorted(timed, key=lambda x: x[:2]):
            stage()
        acc = acc[0]

        phase = lax.rem(it, 2)
        rr_l, pap_l = lanes(rr_acc), lanes(acc)
        T1[it, row] = jnp.concatenate([rr_l, pap_l + RIDGE * rr_l], 0)
        ones = [
            pltpu.make_async_remote_copy(
                src_ref=T1.at[it, row], dst_ref=T1.at[it, row], send_sem=s1_send.at[it, d],
                recv_sem=s1_recv.at[it, d], device_id=(lax.rem(row + d, n_row), col), device_id_type=MESH)
            for d in range(1, n_row)
        ]
        for copy in ones:
            copy.start()

        more = jnp.logical_not(last)

        def rows_of(ref_rows, at):
            return pl.ds(pl.multiple_of(ref_rows.start + at, 32), 32)

        def strip(q):
            return band((2 * odd + q) * h)

        halves = (lefts, rights)
        pieces = [(c, q) for c in (1, 0) for q in range(2)]
        fold_z = {
            (c, q): across(
                once(4 * c + 2 * q), S.at[c, strip(q), top_h], ZR.at[1, c, q], S.at[c, strip(q), end_h],
                ZR.at[0, c, q], z_first[c])
            for c, q in pieces
        }
        fold_x = {
            (c, p): along(once(8 + 2 * c + p), S.at[c, out_halo, halves[p]], RXO.at[c, p], outer_row, x_pair[c])
            for c in range(2) for p in range(2)
        }
        fold_i = along(once(12), S.at[:, inn_halo, :], RXI, inner_row, inner_ok)
        fold_z[1, 0].start()
        fold_x[0, 0].start()
        fold_x[0, 1].start()
        fold_i.start()
        for key in pieces[1:]:
            fold_z[key].start()
        fold_x[1, 0].start()
        fold_x[1, 1].start()

        def meet(index, src, buf, on):
            def slot(p, c0, c1):
                return buf.at[(phase, p) + (slice(None),) * (len(buf.shape) - 3) + (slice(c0, c1),)]

            full, part = jnp.logical_and(on, more), jnp.logical_and(on, last)
            to_left = (
                leftward(turn(index, phase), src(0, side), slot(1, 0, side), full),
                leftward(turn(index, phase), src(0, h), slot(1, 0, h), part))
            to_right = (
                rightward(turn(index + 1, phase), src(side, 2 * side), slot(0, 0, side), full),
                rightward(turn(index + 1, phase), src(3 * h, 4 * h), slot(0, h, side), part))
            return to_left, to_right

        meet_i = meet(0, lambda c0, c1: S.at[:, inn, c0:c1], DXI, yes)
        meet_x = [
            meet(2 + 2 * c, lambda c0, c1, c=c: S.at[c, out, c0:c1], DXO[c], x_first[c]) for c in range(2)
        ]
        meet_z = {
            (c, q): along(
                turn(6 + 2 * c + q, phase), S.at[c, strip(q), own], DZ.at[phase, c, q], outer_row,
                jnp.logical_and(z_first[c], jnp.logical_or(more, odd == q)),
                jnp.logical_and(z_first[c], jnp.logical_or(more, odd != q)))
            for c, q in pieces
        }

        def begin(pair):
            for swap in pair:
                swap.start()

        def end(pair):
            for swap in pair:
                swap.wait()

        fold_i.wait()

        @pl.when(inner_ok)
        def _():
            def add(at):
                S[:, rows_of(inn, at), :] += RXI[:, pl.ds(at, 32), :]
            chunks(h, 32, add)
        begin(meet_i[0])
        begin(meet_i[1])

        def turn_z(c, q):
            fold_z[c, q].wait()
            for ok, cols, side_q in ((left_ok, one, 0), (right_ok, two, 1)):
                @pl.when(jnp.logical_and(z_first[c], ok))
                def _():
                    def add(at):
                        S[c, rows_of(strip(q), at), cols] += ZR[side_q, c, q, pl.ds(at, 32), :]
                    chunks(h, 32, add)
            meet_z[c, q].start()

        def turn_x(c):
            for p in range(2):
                fold_x[c, p].wait()

                @pl.when(x_pair[c])
                def _():
                    def add(at):
                        S[c, rows_of(out, at), halves[p]] += RXO[c, p, pl.ds(at, 32), :]
                    chunks(h, 32, add)
                begin(meet_x[c][p])

        turn_z(*pieces[0])
        turn_z(*pieces[1])
        turn_x(0)
        for copy in ones:
            copy.wait()
        total = T1[it, 0]
        for q in range(1, n_row):
            total = total + T1[it, q]
        T2[it, col] = total
        twos = [
            pltpu.make_async_remote_copy(
                src_ref=T2.at[it, col], dst_ref=T2.at[it, col], send_sem=s2_send.at[it, d],
                recv_sem=s2_recv.at[it, d], device_id=(row, lax.rem(col + d, n_col)), device_id_type=MESH)
            for d in range(1, n_col)
        ]
        for copy in twos:
            copy.start()
        turn_z(*pieces[2])
        turn_z(*pieces[3])
        turn_x(1)

        def settle(c, rows, p, got):
            ok, cols, mine = ((left_ok, lefts, one), (right_ok, rights, two))[p]

            @pl.when(ok)
            def _():
                def run(at):
                    here = rows_of(rows, at)
                    G[c, here, cols] = S[c, here, cols] + got(pl.ds(at, 32))
                chunks(h, 32, run)

            @pl.when(jnp.logical_not(ok))
            def _():
                def run(at):
                    here = rows_of(rows, at)
                    G[c, here, mine] = S[c, here, mine]
                chunks(h, 32, run)

        shares = []

        def share(swap):
            swap.start()
            shares.append(swap)

        def done_i(p):
            end(meet_i[1 - p])
            for c in range(2):
                settle(c, inn, p, lambda there, c=c: DXI[phase, p, c, there, :])
            share(along(once(16 + p), G.at[:, inn, halves[p]], G.at[:, inn_there, halves[p]], inner_row,
                        jnp.logical_and(inner_ok, more)))

        def done_x(c, p):
            end(meet_x[c][1 - p])

            @pl.when(x_first[c])
            def _():
                settle(c, out, p, lambda there: DXO[c][phase, p, there, :])
            share(along(once(18 + 2 * c + p), G.at[c, out, halves[p]], G.at[c, out_there, halves[p]], outer_row,
                        jnp.logical_and(x_pair[c], more)))

        def done_z(c, q):
            meet_z[c, q].wait()

            @pl.when(z_first[c])
            def _():
                def run(at):
                    here = rows_of(strip(q), at)
                    G[c, here, own] = S[c, here, own] + DZ[phase, c, q, pl.ds(at, 32), :]
                chunks(h, 32, run)
            share(across(
                once(22 + 4 * c + 2 * q), G.at[c, strip(q), one], G.at[c, strip(q), end_h],
                G.at[c, strip(q), two], G.at[c, strip(q), top_h], jnp.logical_and(z_first[c], more)))

        done_z(*pieces[0])
        done_i(0)
        done_i(1)
        done_x(0, 0)
        done_x(0, 1)
        for key in pieces[1:]:
            done_z(*key)
        done_x(1, 0)
        done_x(1, 1)

        for copy in twos:
            copy.wait()
        total = T2[it, 0]
        for q in range(1, n_col):
            total = total + T2[it, q]
        rr = jnp.sum(total[0:1], keepdims=True)
        pap = jnp.sum(total[1:2], keepdims=True)
        ratio = jnp.where(it == 0, 0.0, rr / rr_before)
        alpha = rr / (pap - ratio * rr / alpha_before)

        def advance(i, carry):
            near = pl.ds(pl.multiple_of(i * 32, 32), 32)
            rows = pl.ds(pl.multiple_of(h + i * 32, 32), 32)
            for c in range(2):
                d = R[c, rows, own] + ratio * D[c, near, :]
                D[c, near, :] = d
                SOL[c, near, :] += alpha * d
            return carry
        lax.fori_loop(0, side // 32, advance, 0)

        for swap in shares:
            swap.wait()

        @pl.when(more)
        def _():
            def advance_r(at):
                rows = pl.ds(at, 32)
                for c in range(2):
                    r = R[c, rows, :]
                    image = G[c, rows, :] + RIDGE * r + ratio * L[c, rows, :]
                    L[c, rows, :] = image
                    R[c, rows, :] = r - alpha * image
            chunks(2 * side, 32, advance_r)

        @pl.when(last)
        def _():
            def emit(at):
                rows = pl.ds(pl.multiple_of(h + at, 32), 32)
                for c in range(2):
                    r = R[c, rows, own]
                    image = G[c, rows, own] + RIDGE * r + ratio * L[c, rows, own]
                    res_ref[c, pl.ds(at, 32), :] = r - alpha * image
            chunks(side, 32, emit)
        return alpha, rr

    one11 = jnp.ones((1, 1), F32)
    lax.fori_loop(0, ITERS, iteration, (one11, one11))


def solution(mesh):
    n_row, n_col = mesh.shape["row"], mesh.shape["col"]
    n_x = len({tuple(getattr(d, "coords", (d.id,)))[0] for d in mesh.devices.flat})

    def local(right_side, probe, weights, offsets, counts):
        side = probe.shape[1]
        cap = offsets.shape[2]
        h = side // 2
        mats = jnp.asarray(tables(side))
        block = jax.ShapeDtypeStruct((2, side, side), F32)
        hbm = pl.BlockSpec(memory_space=pltpu.HBM)
        smem = pl.BlockSpec(memory_space=pltpu.SMEM)
        wide = pltpu.VMEM((2, 2 * side, 2 * side), F32)
        tile = pltpu.VMEM((2, side, side), F32)
        dma = pltpu.SemaphoreType.DMA
        vmem = pl.BlockSpec(memory_space=pltpu.VMEM)
        return pl.pallas_call(
            functools.partial(kernel, n_row, n_col, n_x, cap, side),
            out_shape=(block, block),
            in_specs=[smem, smem, hbm, hbm, hbm, hbm],
            out_specs=(vmem, vmem),
            scratch_shapes=[
                wide, wide, wide, wide,
                tile,
                pltpu.VMEM((cap, 2, side, side), F32),
                tile,
                pltpu.VMEM((side, side), F32),
                pltpu.VMEM((8, side, side), BF16),
                [pltpu.VMEM((4, 2, side, side), BF16) for _ in range(cap)],
                [pltpu.VMEM((4, side, side), F32) for _ in range(cap)],
                tile,
                pltpu.VMEM((2, h, 2 * side), F32),
                pltpu.VMEM((2, 2, h, side), F32),
                pltpu.VMEM((2, 2, 2, h, side), F32),
                [pltpu.VMEM((2, 2, h, side), F32) for _ in range(2)],
                pltpu.VMEM((2, 2, 2, h, h), F32),
                pltpu.VMEM((2, 2, 2, h, side), F32),
                pltpu.VMEM((ITERS, n_row, 2, 128), F32),
                pltpu.VMEM((ITERS, n_col, 2, 128), F32),
                dma((48,)), dma((48,)), dma((2, 10)), dma((2, 10)),
                dma((ITERS, n_row)), dma((ITERS, n_row)),
                dma((ITERS, n_col)), dma((ITERS, n_col)),
                dma((4,)),
            ],
            compiler_params=pltpu.CompilerParams(
                collective_id=0, has_side_effects=True, vmem_limit_bytes=53824 * 1024),
        )(offsets[0, 0].T, counts, right_side, probe, weights, mats)

    placed = (P(None, "row", "col"), P(), P(), P("row", "col", None, None), P("row", "col"))
    return jax.shard_map(
        local, mesh=mesh, in_specs=placed, out_specs=(P(None, "row", "col"), P(None, "row", "col")), check_vma=False)
```

```python
import functools
import math

import jax
import jax.numpy as jnp
import numpy as np
from jax import lax
from jax.experimental import pallas as pl
from jax.experimental.pallas import tpu as pltpu
from jax.sharding import PartitionSpec as P

ITERS = 3
RIDGE = 0.5
SKEW = 0.1
STRIPS = 2
MESH = pl.DeviceIdType.MESH
F32 = jnp.float32
BF16 = jnp.bfloat16


def tables(length):
    half = length // 2
    k = np.arange(half)[:, None]
    n = np.arange(half)[None, :]
    out = []
    for odd in (0, 1):
        angle = 2.0 * math.pi * ((n * (2 * k + odd)) % length) / length
        re, im = np.cos(angle) / math.sqrt(length), -np.sin(angle) / math.sqrt(length)
        real = np.block([[re, -im], [im, re]])
        for mat in (real, real.T):
            hi = mat.astype(BF16)
            out += [hi, (mat - hi.astype(np.float64)).astype(BF16)]
    return np.stack(out)


def kernel(
    n_row, n_col, n_x, cap, side,
    off_ref, cnt_ref, rhs_hbm, probe_hbm, w_hbm, mat_hbm,
    SOL, res_ref,
    R, G, L, S, D, PR, P0, W0, mat_ref, XS, YS, W, RXI, RXO, DXI, DXO, ZR, DZ, T1, T2,
    one_send, one_recv, two_send, two_recv, s1_send, s1_recv, s2_send, s2_recv, io_sem,
):
    h = side // 2
    own = slice(h, h + side)
    row = lax.axis_index("row")
    col = lax.axis_index("col")

    load_r = pltpu.make_async_copy(rhs_hbm, R.at[:, own, own], io_sem.at[0])
    load_p = pltpu.make_async_copy(probe_hbm, P0, io_sem.at[1])
    load_w = pltpu.make_async_copy(w_hbm, W0, io_sem.at[2])
    load_m = pltpu.make_async_copy(mat_hbm, mat_ref, io_sem.at[3])
    for load in (load_r, load_p, load_w, load_m):
        load.start()

    def chunks(total, step, body):
        def run(i, carry):
            body(pl.multiple_of(i * step, step))
            return carry
        lax.fori_loop(0, total // step, run, 0)

    def fill(buf, rows, cols):
        def run(at):
            buf[:, pl.ds(pl.multiple_of(rows.start + at, 32), 32), cols] = jnp.zeros(
                (2, 32, cols.stop - cols.start), F32)
        chunks(rows.stop - rows.start, 32, run)

    every = slice(0, 2 * side)
    one, two, top_h, end_h = slice(h, 2 * h), slice(2 * h, 3 * h), slice(0, h), slice(3 * h, 4 * h)
    lefts, rights = slice(0, side), slice(side, 2 * side)
    left_ok, right_ok = col > 0, col < n_col - 1
    pl.when(row == 0)(lambda: fill(R, top_h, every))
    pl.when(row == n_row - 1)(lambda: fill(R, end_h, every))
    pl.when(col == 0)(lambda: fill(R, every, top_h))
    pl.when(col == n_col - 1)(lambda: fill(R, every, end_h))

    barrier = pltpu.get_barrier_semaphore()
    for d in range(1, n_row):
        pl.semaphore_signal(barrier, inc=1, device_id=(lax.rem(row + d, n_row), col), device_id_type=MESH)
    for d in range(1, n_col):
        pl.semaphore_signal(barrier, inc=1, device_id=(row, lax.rem(col + d, n_col)), device_id_type=MESH)
    pl.semaphore_wait(barrier, n_row - 1 + n_col - 1)

    odd = lax.rem(row, 2)
    inner_row = row + 1 - 2 * odd
    outer_row = row - 1 + 2 * odd
    inner_ok = inner_row < n_row
    outer_ok = jnp.logical_and(outer_row >= 0, outer_row < n_row)
    bent = lax.rem((row + 1) // 2, n_x) == 0
    z_first = (jnp.logical_and(bent, outer_ok), outer_ok)
    x_first = tuple(jnp.logical_not(z) for z in z_first)
    x_pair = tuple(jnp.logical_and(x, outer_ok) for x in x_first)

    def band(start, size=h):
        return pl.ds(pl.multiple_of(start, h), size)

    inn, inn_halo, inn_there = band((2 - odd) * h), band(3 * h * (1 - odd)), band(3 * h * odd)
    out, out_halo, out_there = band((1 + odd) * h), band(3 * h * odd), band(3 * h * (1 - odd))
    outer = band(2 * h * odd, side)

    class Swap:
        def __init__(self, sems, parts):
            send, recv = sems
            self.parts = []
            for q, (src, dst, device, sends, gets) in enumerate(parts):
                self.parts.append((pltpu.make_async_remote_copy(
                    src_ref=src, dst_ref=dst, send_sem=send(q), recv_sem=recv(q),
                    device_id=device, device_id_type=MESH), sends, gets))

        def start(self):
            for copy, sends, _ in self.parts:
                pl.when(sends)(copy.start)

        def wait(self):
            for copy, sends, gets in self.parts:
                pl.when(sends)(copy.wait_send)
                pl.when(gets)(copy.wait_recv)

    def once(index):
        return (lambda q: one_send.at[index + q]), (lambda q: one_recv.at[index + q])

    def turn(index, phase):
        return (lambda q: two_send.at[phase, index + q]), (lambda q: two_recv.at[phase, index + q])

    def across(sems, left_src, left_dst, right_src, right_dst, on):
        go_left, go_right = jnp.logical_and(on, left_ok), jnp.logical_and(on, right_ok)
        return Swap(sems, [
            (left_src, left_dst, (row, col - 1), go_left, go_right),
            (right_src, right_dst, (row, col + 1), go_right, go_left)])

    def leftward(sems, src, dst, on):
        return Swap(sems, [(src, dst, (row, col - 1), jnp.logical_and(on, left_ok), jnp.logical_and(on, right_ok))])

    def rightward(sems, src, dst, on):
        return Swap(sems, [(src, dst, (row, col + 1), jnp.logical_and(on, right_ok), jnp.logical_and(on, left_ok))])

    def along(sems, src, dst, there, on, gets=None):
        return Swap(sems, [(src, dst, (there, col), on, on if gets is None else gets)])

    yes = col >= 0

    def spread(F):
        ends = [
            across(once(30 + 2 * c), F.at[c, out, one], F.at[c, out, end_h], F.at[c, out, two], F.at[c, out, top_h], yes)
            for c in range(2)
        ]
        mids = across(once(34), F.at[:, inn, one], F.at[:, inn, end_h], F.at[:, inn, two], F.at[:, inn, top_h], yes)
        firsts = [along(once(36 + c), F.at[c, out, own], F.at[c, out_there, own], outer_row, z_first[c]) for c in range(2)]
        ends[0].start()
        firsts[1].start()
        firsts[0].start()
        mids.start()
        ends[1].start()
        laters = []
        ends[0].wait()
        laters.append(along(once(38), F.at[0, out, :], F.at[0, out_there, :], outer_row, x_pair[0]))
        laters[-1].start()
        for c in (1, 0):
            firsts[c].wait()
            laters.append(across(
                once(40 + 2 * c), F.at[c, out_halo, one], F.at[c, out_halo, end_h],
                F.at[c, out_halo, two], F.at[c, out_halo, top_h], z_first[c]))
            laters[-1].start()
        mids.wait()
        laters.append(along(once(44), F.at[:, inn, :], F.at[:, inn_there, :], inner_row, inner_ok))
        laters[-1].start()
        ends[1].wait()

        def wait():
            for swap in laters:
                swap.wait()

        return wait

    load_r.wait()
    spread_wait = spread(R)

    fill(G, every, every)
    fill(L, every, every)
    for buf in (D, SOL):
        fill(buf, slice(0, buf.shape[1]), slice(0, buf.shape[2]))

    load_p.wait()
    for s in range(cap):
        on = jnp.where(s < cnt_ref[0, 0], 1.0, 0.0).astype(F32)
        for c in range(2):
            rolled = pltpu.roll(P0[c], off_ref[0, s] + h, 0)
            PR[s, c] = pltpu.roll(rolled, off_ref[1, s] + h, 1) * on

    def three(val):
        top = val.astype(BF16)
        rest = val - top.astype(F32)
        mid = rest.astype(BF16)
        return top, mid, (rest - mid.astype(F32)).astype(BF16)

    load_w.wait()
    first = lax.broadcasted_iota(jnp.int32, (side, side), 0)
    second = lax.broadcasted_iota(jnp.int32, (side, side), 1)
    freq = jnp.where(first >= h, 2 * (first - h) + 1, 2 * first)
    pick = jnp.where(second == freq, 1.0, 0.0).astype(BF16)
    by_row = sum(jnp.dot(pick, part, preferred_element_type=F32) for part in three(W0[...]))
    parts = three(by_row)
    lane = jnp.where(second >= h, second - h, second)
    for q in range(2):
        pick = jnp.where(first == 2 * lane + q, 1.0, 0.0).astype(BF16)
        W[q] = sum(jnp.dot(part, pick, preferred_element_type=F32) for part in parts)

    load_m.wait()
    spread_wait()

    step = 32

    def fold(val):
        return jnp.sum(val.reshape(-1, 8, val.shape[-1]), axis=0)

    sub = lax.broadcasted_iota(jnp.int32, (step, h), 0)
    lan = lax.broadcasted_iota(jnp.int32, (step, h), 1)

    def side_of(s, at):
        if s == 0:
            return "both" if at < h else "near"
        if s == 1:
            return "far" if at < h else "both"
        return "both"

    def patch(s, k, seen, acc):
        X, Y = XS[k], YS[k]
        a = off_ref[0, s] + h
        b = off_ref[1, s] + h

        def put(j, rows, val):
            hi = val.astype(BF16)
            X[j, 0, rows, :] = hi
            X[j, 1, rows, :] = (val - hi.astype(F32)).astype(BF16)

        def left(m, j):
            hi, lo = mat_ref[m], mat_ref[m + 1]
            xh, xl = X[j, 0], X[j, 1]
            return jnp.dot(
                jnp.concatenate([hi, lo, hi], 1), jnp.concatenate([xh, xh, xl], 0), preferred_element_type=F32)

        def right(j, m):
            hi, lo = mat_ref[m], mat_ref[m + 1]
            xh, xl = X[j, 0], X[j, 1]
            return jnp.dot(
                jnp.concatenate([xh, xl, xh], 1), jnp.concatenate([hi, hi, lo], 0), preferred_element_type=F32)

        def covered(c, base):
            halves = []
            for at in (0, h):
                cols, fcols = slice(at, at + h), slice(side + at, side + at + h)
                rk, ck = side_of(s, base), side_of(s, at)
                rows, far = slice(base, base + step), slice(side + base, side + base + step)

                def in_cols(r):
                    if ck == "near":
                        return R[c, r, cols]
                    if ck == "far":
                        return R[c, r, fcols]
                    return jnp.where(lan + at >= b, R[c, r, cols], R[c, r, fcols])

                if rk == "near":
                    halves.append(in_cols(rows))
                elif rk == "far":
                    halves.append(in_cols(far))
                else:
                    halves.append(jnp.where(sub + base >= a, in_cols(rows), in_cols(far)))
            return jnp.concatenate(halves, 1)

        def scatter(c, base, term):
            for at in (0, h):
                val = term[:, at:at + h]
                rk, ck = side_of(s, base), side_of(s, at)
                rows = {}
                if rk == "both":
                    near = jnp.where(sub + base >= a, val, 0.0)
                    rows = {0: near, side: val - near}
                else:
                    rows = {0 if rk == "near" else side: val}
                for shift, part in rows.items():
                    if ck == "both":
                        near = jnp.where(lan + at >= b, part, 0.0)
                        cells = {0: near, side: part - near}
                    else:
                        cells = {0 if ck == "near" else side: part}
                    for over, cell in cells.items():
                        r0, c0 = shift + base, over + at
                        where = (c, slice(r0, r0 + step), slice(c0, c0 + h))
                        if (c, r0, c0) in seen:
                            S[where] += cell
                        else:
                            S[where] = cell
                            seen.add((c, r0, c0))

        def load():
            for t in range(0, h, step):
                parts = []
                for base in (t, h + t):
                    rows = slice(base, base + step)
                    v = [covered(c, base) for c in range(2)]
                    p0, p1 = PR[s, 0, rows, :], PR[s, 1, rows, :]
                    parts.append((p0 * v[0] - p1 * v[1], p0 * v[1] + p1 * v[0]))
                for c in range(2):
                    rows = slice(c * h + t, c * h + t + step)
                    put(0, rows, parts[0][c] + parts[1][c])
                    put(1, rows, parts[0][c] - parts[1][c])

        def mul_a():
            Y[0] = left(0, 0)
            Y[1] = left(4, 1)

        def mix_b():
            for j in range(2):
                for t in range(0, h, step):
                    re, im = Y[j, t:t + step, :], Y[j, h + t:h + t + step, :]
                    rows = slice(j * h + t, j * h + t + step)
                    put(2, rows, jnp.concatenate([re[:, :h] + re[:, h:], im[:, :h] + im[:, h:]], 1))
                    put(3, rows, jnp.concatenate([re[:, :h] - re[:, h:], im[:, :h] - im[:, h:]], 1))

        def mul_b():
            Y[2] = right(2, 2)
            Y[3] = right(3, 6)

        def mix_c():
            for j in range(2):
                for t in range(0, side, step):
                    rows = slice(t, t + step)
                    f = Y[2 + j, rows, :]
                    wf = W[j, rows, :] * f
                    acc[0] = acc[0] + fold(wf * f)
                    put(j, rows, wf)

        def mul_c():
            Y[0] = right(0, 0)
            Y[1] = right(1, 4)

        def mix_d():
            for j in range(2):
                for t in range(0, h, step):
                    rows = slice(j * h + t, j * h + t + step)
                    c, d = Y[0, rows, :], Y[1, rows, :]
                    p, m = c + d, c - d
                    put(2 + j, slice(t, t + step), jnp.concatenate([p[:, :h], m[:, :h]], 1))
                    put(2 + j, slice(h + t, h + t + step), jnp.concatenate([p[:, h:], m[:, h:]], 1))

        def mul_d():
            Y[2] = left(2, 2)
            Y[3] = left(6, 3)

        def store():
            for t in range(0, h, step):
                for sign, base in ((1, t), (-1, h + t)):
                    rows = slice(base, base + step)
                    if sign == 1:
                        hr = Y[2, t:t + step, :] + Y[3, t:t + step, :]
                        hi = Y[2, h + t:h + t + step, :] + Y[3, h + t:h + t + step, :]
                    else:
                        hr = Y[2, t:t + step, :] - Y[3, t:t + step, :]
                        hi = Y[2, h + t:h + t + step, :] - Y[3, h + t:h + t + step, :]
                    p0, p1 = PR[s, 0, rows, :], PR[s, 1, rows, :]
                    scatter(0, base, p0 * hr + p1 * hi)
                    scatter(1, base, p0 * hi - p1 * hr)

        return [load, mul_a, mix_b, mul_b, mix_c, mul_c, mix_d, mul_d, store]

    def lanes(acc):
        total = acc[:, 0:128]
        for q in range(128, acc.shape[1], 128):
            total = total + acc[:, q:q + 128]
        return jnp.sum(total, axis=0, keepdims=True)

    def iteration(it, carry):
        alpha_before, rr_before = carry
        last = it + 1 == ITERS

        def norm(i, acc):
            v = R[:, pl.ds(pl.multiple_of(h + i * 32, 32), 32), own]
            return acc + fold(v[0] * v[0]) + fold(v[1] * v[1])
        rr_acc = lax.fori_loop(0, side // 32, norm, jnp.zeros((8, side), F32))

        order = [*range(2, cap), 0, 1]
        seen = set()
        acc = [jnp.zeros((8, side), F32)]
        timed = []
        for n, s in enumerate(order):
            for q, stage in enumerate(patch(s, n, seen, acc)):
                timed.append((SKEW * n + q, n, stage))
        for _, _, stage in sorted(timed, key=lambda x: x[:2]):
            stage()
        acc = acc[0]

        phase = lax.rem(it, 2)
        rr_l, pap_l = lanes(rr_acc), lanes(acc)
        T1[it, row] = jnp.concatenate([rr_l, pap_l + RIDGE * rr_l], 0)
        ones = [
            pltpu.make_async_remote_copy(
                src_ref=T1.at[it, row], dst_ref=T1.at[it, row], send_sem=s1_send.at[it, d],
                recv_sem=s1_recv.at[it, d], device_id=(lax.rem(row + d, n_row), col), device_id_type=MESH)
            for d in range(1, n_row)
        ]
        for copy in ones:
            copy.start()

        more = jnp.logical_not(last)

        def rows_of(ref_rows, at):
            return pl.ds(pl.multiple_of(ref_rows.start + at, 32), 32)

        tall = side // STRIPS

        def strip(q):
            return pl.ds(pl.multiple_of(2 * h * odd + q * tall, tall), tall)

        halves = (lefts, rights)
        pieces = [(c, q) for c in (1, 0) for q in range(STRIPS)]
        fold_z = {
            (c, q): across(
                once(48 + 2 * (c * STRIPS + q)), S.at[c, strip(q), top_h], ZR.at[1, c, q], S.at[c, strip(q), end_h],
                ZR.at[0, c, q], z_first[c])
            for c, q in pieces
        }
        fold_x = {
            (c, p): along(once(8 + 2 * c + p), S.at[c, out_halo, halves[p]], RXO.at[c, p], outer_row, x_pair[c])
            for c in range(1) for p in range(2)
        }
        fold_i = along(once(12), S.at[:, inn_halo, :], RXI, inner_row, inner_ok)
        fold_z[1, 0].start()
        fold_x[0, 0].start()
        fold_x[0, 1].start()
        fold_i.start()
        for key in pieces[1:]:
            fold_z[key].start()

        def meet(index, src, buf, on):
            def slot(p, c0, c1):
                return buf.at[(phase, p) + (slice(None),) * (len(buf.shape) - 3) + (slice(c0, c1),)]

            full, part = jnp.logical_and(on, more), jnp.logical_and(on, last)
            to_left = (
                leftward(turn(index, phase), src(0, side), slot(1, 0, side), full),
                leftward(turn(index, phase), src(0, h), slot(1, 0, h), part))
            to_right = (
                rightward(turn(index + 1, phase), src(side, 2 * side), slot(0, 0, side), full),
                rightward(turn(index + 1, phase), src(3 * h, 4 * h), slot(0, h, side), part))
            return to_left, to_right

        meet_i = meet(0, lambda c0, c1: S.at[:, inn, c0:c1], DXI, yes)
        meet_x = [
            meet(2 + 2 * c, lambda c0, c1, c=c: S.at[c, out, c0:c1], DXO[c], x_first[c]) for c in range(2)
        ]
        meet_z = {
            (c, q): along(
                turn(6 + c * STRIPS + q, phase), S.at[c, strip(q), own], DZ.at[phase, c, q], outer_row,
                jnp.logical_and(z_first[c], jnp.logical_or(more, odd == 2 * q // STRIPS)),
                jnp.logical_and(z_first[c], jnp.logical_or(more, odd != 2 * q // STRIPS)))
            for c, q in pieces
        }

        def begin(pair):
            for swap in pair:
                swap.start()

        def end(pair):
            for swap in pair:
                swap.wait()

        fold_i.wait()

        @pl.when(inner_ok)
        def _():
            def add(at):
                S[:, rows_of(inn, at), :] += RXI[:, pl.ds(at, 32), :]
            chunks(h, 32, add)
        begin(meet_i[0])
        begin(meet_i[1])

        def turn_z(c, q):
            fold_z[c, q].wait()
            for ok, cols, side_q in ((left_ok, one, 0), (right_ok, two, 1)):
                @pl.when(jnp.logical_and(z_first[c], ok))
                def _():
                    def add(at):
                        S[c, rows_of(strip(q), at), cols] += ZR[side_q, c, q, pl.ds(at, 32), :]
                    chunks(tall, 32, add)
            meet_z[c, q].start()

        def turn_x(c):
            for p in range(2):
                if c == 0:
                    fold_x[c, p].wait()

                    @pl.when(x_pair[c])
                    def _():
                        def add(at):
                            S[c, rows_of(out, at), halves[p]] += RXO[c, p, pl.ds(at, 32), :]
                        chunks(h, 32, add)
                begin(meet_x[c][p])

        for key in pieces[:STRIPS]:
            turn_z(*key)
        turn_x(0)
        for copy in ones:
            copy.wait()
        total = T1[it, 0]
        for q in range(1, n_row):
            total = total + T1[it, q]
        T2[it, col] = total
        twos = [
            pltpu.make_async_remote_copy(
                src_ref=T2.at[it, col], dst_ref=T2.at[it, col], send_sem=s2_send.at[it, d],
                recv_sem=s2_recv.at[it, d], device_id=(row, lax.rem(col + d, n_col)), device_id_type=MESH)
            for d in range(1, n_col)
        ]
        for copy in twos:
            copy.start()
        for key in pieces[STRIPS:]:
            turn_z(*key)
        turn_x(1)

        def settle(c, rows, p, got):
            ok, cols, mine = ((left_ok, lefts, one), (right_ok, rights, two))[p]

            @pl.when(ok)
            def _():
                def run(at):
                    here = rows_of(rows, at)
                    G[c, here, cols] = S[c, here, cols] + got(pl.ds(at, 32))
                chunks(h, 32, run)

            @pl.when(jnp.logical_not(ok))
            def _():
                def run(at):
                    here = rows_of(rows, at)
                    G[c, here, mine] = S[c, here, mine]
                chunks(h, 32, run)

        shares = []

        def share(swap):
            swap.start()
            shares.append(swap)

        def done_i(p):
            end(meet_i[1 - p])
            for c in range(2):
                settle(c, inn, p, lambda there, c=c: DXI[phase, p, c, there, :])
            share(along(once(16 + p), G.at[:, inn, halves[p]], G.at[:, inn_there, halves[p]], inner_row,
                        jnp.logical_and(inner_ok, more)))

        def done_x(c, p):
            end(meet_x[c][1 - p])

            @pl.when(x_first[c])
            def _():
                settle(c, out, p, lambda there: DXO[c][phase, p, there, :])
            if c == 0:
                share(along(once(18 + 2 * c + p), G.at[c, out, halves[p]], G.at[c, out_there, halves[p]], outer_row,
                            jnp.logical_and(x_pair[c], more)))

        def done_z(c, q):
            meet_z[c, q].wait()

            @pl.when(z_first[c])
            def _():
                def run(at):
                    here = rows_of(strip(q), at)
                    G[c, here, own] = S[c, here, own] + DZ[phase, c, q, pl.ds(at, 32), :]
                chunks(tall, 32, run)
            share(across(
                once(48 + 4 * STRIPS + 2 * (c * STRIPS + q)), G.at[c, strip(q), one], G.at[c, strip(q), end_h],
                G.at[c, strip(q), two], G.at[c, strip(q), top_h], jnp.logical_and(z_first[c], more)))

        for key in pieces[:STRIPS]:
            done_z(*key)
        done_i(0)
        done_i(1)
        done_x(0, 0)
        done_x(0, 1)
        for key in pieces[STRIPS:]:
            done_z(*key)
        done_x(1, 0)
        done_x(1, 1)

        for copy in twos:
            copy.wait()
        total = T2[it, 0]
        for q in range(1, n_col):
            total = total + T2[it, q]
        rr = jnp.sum(total[0:1], keepdims=True)
        pap = jnp.sum(total[1:2], keepdims=True)
        ratio = jnp.where(it == 0, 0.0, rr / rr_before)
        alpha = rr / (pap - ratio * rr / alpha_before)

        def update(rows, cols):
            for c in range(2):
                r = R[c, rows, cols]
                image = G[c, rows, cols] + RIDGE * r + ratio * L[c, rows, cols]
                L[c, rows, cols] = image
                R[c, rows, cols] = r - alpha * image

        def advance(i, carry):
            near = pl.ds(pl.multiple_of(i * 32, 32), 32)
            rows = pl.ds(pl.multiple_of(h + i * 32, 32), 32)
            for c in range(2):
                d = R[c, rows, own] + ratio * D[c, near, :]
                D[c, near, :] = d
                SOL[c, near, :] += alpha * d
            return carry
        lax.fori_loop(0, side // 32, advance, 0)

        @pl.when(more)
        def _():
            def advance_own(at):
                rows = pl.ds(pl.multiple_of(h + at, 32), 32)
                update(rows, own)
            chunks(side, 32, advance_own)
        for swap in shares:
            swap.wait()

        @pl.when(more)
        def _():
            def advance_r(at):
                update(pl.ds(pl.multiple_of(at, 32), 32), every)
                update(pl.ds(pl.multiple_of(3 * h + at, 32), 32), every)
                for shift in (h, 2 * h):
                    update(pl.ds(pl.multiple_of(shift + at, 32), 32), top_h)
                    update(pl.ds(pl.multiple_of(shift + at, 32), 32), end_h)
            chunks(h, 32, advance_r)

        @pl.when(last)
        def _():
            def emit(at):
                rows = pl.ds(pl.multiple_of(h + at, 32), 32)
                for c in range(2):
                    r = R[c, rows, own]
                    image = G[c, rows, own] + RIDGE * r + ratio * L[c, rows, own]
                    res_ref[c, pl.ds(at, 32), :] = r - alpha * image
            chunks(side, 32, emit)
        return alpha, rr

    one11 = jnp.ones((1, 1), F32)
    lax.fori_loop(0, ITERS, iteration, (one11, one11))


def solution(mesh):
    n_row, n_col = mesh.shape["row"], mesh.shape["col"]
    n_x = len({tuple(getattr(d, "coords", (d.id,)))[0] for d in mesh.devices.flat})

    def local(right_side, probe, weights, offsets, counts):
        side = probe.shape[1]
        cap = offsets.shape[2]
        h = side // 2
        mats = jnp.asarray(tables(side))
        weights = pltpu.with_memory_space_constraint(weights, pltpu.HBM)
        block = jax.ShapeDtypeStruct((2, side, side), F32)
        hbm = pl.BlockSpec(memory_space=pltpu.HBM)
        smem = pl.BlockSpec(memory_space=pltpu.SMEM)
        wide = pltpu.VMEM((2, 2 * side, 2 * side), F32)
        tile = pltpu.VMEM((2, side, side), F32)
        dma = pltpu.SemaphoreType.DMA
        vmem = pl.BlockSpec(memory_space=pltpu.VMEM)
        return pl.pallas_call(
            functools.partial(kernel, n_row, n_col, n_x, cap, side),
            out_shape=(block, block),
            in_specs=[smem, smem, hbm, hbm, hbm, hbm],
            out_specs=(vmem, vmem),
            scratch_shapes=[
                wide, wide, wide, wide,
                tile,
                pltpu.VMEM((cap, 2, side, side), F32),
                tile,
                pltpu.VMEM((side, side), F32),
                pltpu.VMEM((8, side, side), BF16),
                [pltpu.VMEM((4, 2, side, side), BF16) for _ in range(cap)],
                [pltpu.VMEM((4, side, side), F32) for _ in range(cap)],
                tile,
                pltpu.VMEM((2, h, 2 * side), F32),
                pltpu.VMEM((2, 2, h, side), F32),
                pltpu.VMEM((2, 2, 2, h, side), F32),
                [pltpu.VMEM((2, 2, h, side), F32) for _ in range(2)],
                pltpu.VMEM((2, 2, STRIPS, side // STRIPS, h), F32),
                pltpu.VMEM((2, 2, STRIPS, side // STRIPS, side), F32),
                pltpu.VMEM((ITERS, n_row, 2, 128), F32),
                pltpu.VMEM((ITERS, n_col, 2, 128), F32),
                dma((48 + 8 * STRIPS,)), dma((48 + 8 * STRIPS,)), dma((2, 6 + 2 * STRIPS)), dma((2, 6 + 2 * STRIPS)),
                dma((ITERS, n_row)), dma((ITERS, n_row)),
                dma((ITERS, n_col)), dma((ITERS, n_col)),
                dma((4,)),
            ],
            compiler_params=pltpu.CompilerParams(
                collective_id=0, has_side_effects=True, vmem_limit_bytes=53824 * 1024),
        )(pltpu.with_memory_space_constraint(offsets[0, 0].T, pltpu.HBM), counts, right_side, probe, weights, mats)

    placed = (P(None, "row", "col"), P(), P(), P("row", "col", None, None), P("row", "col"))
    return jax.shard_map(
        local, mesh=mesh, in_specs=placed, out_specs=(P(None, "row", "col"), P(None, "row", "col")), check_vma=False)
```

```python
import functools
import math

import jax
import jax.numpy as jnp
import numpy as np
from jax import lax
from jax.experimental import pallas as pl
from jax.experimental.pallas import tpu as pltpu
from jax.sharding import PartitionSpec as P

ITERS = 3
RIDGE = 0.5
SKEW = 0.1
STRIPS = 2
MESH = pl.DeviceIdType.MESH
F32 = jnp.float32
BF16 = jnp.bfloat16


def tables(length):
    half = length // 2
    k = np.arange(half)[:, None]
    n = np.arange(half)[None, :]
    out = []
    for odd in (0, 1):
        angle = 2.0 * math.pi * ((n * (2 * k + odd)) % length) / length
        re, im = np.cos(angle) / math.sqrt(length), -np.sin(angle) / math.sqrt(length)
        real = np.block([[re, -im], [im, re]])
        for mat in (real, real.T):
            hi = mat.astype(BF16)
            out += [hi, (mat - hi.astype(np.float64)).astype(BF16)]
    return np.stack(out)


def kernel(
    n_row, n_col, n_x, cap, side,
    off_ref, cnt_ref, rhs_hbm, probe_hbm, w_hbm, mat_hbm,
    SOL, res_ref,
    R, G, L, S, D, PR, P0, W0, mat_ref, XS, YS, W, RXI, RXO, DXI, DXO, ZR, DZ, T1, T2,
    one_send, one_recv, two_send, two_recv, s1_send, s1_recv, s2_send, s2_recv, io_sem,
):
    h = side // 2
    own = slice(h, h + side)
    row = lax.axis_index("row")
    col = lax.axis_index("col")

    load_r = pltpu.make_async_copy(rhs_hbm, R.at[:, own, own], io_sem.at[0])
    load_p = pltpu.make_async_copy(probe_hbm, P0, io_sem.at[1])
    load_w = pltpu.make_async_copy(w_hbm, W0, io_sem.at[2])
    load_m = pltpu.make_async_copy(mat_hbm, mat_ref, io_sem.at[3])
    for load in (load_r, load_p, load_w, load_m):
        load.start()

    def chunks(total, step, body):
        def run(i, carry):
            body(pl.multiple_of(i * step, step))
            return carry
        lax.fori_loop(0, total // step, run, 0)

    def fill(buf, rows, cols):
        def run(at):
            buf[:, pl.ds(pl.multiple_of(rows.start + at, 32), 32), cols] = jnp.zeros(
                (2, 32, cols.stop - cols.start), F32)
        chunks(rows.stop - rows.start, 32, run)

    every = slice(0, 2 * side)
    one, two, top_h, end_h = slice(h, 2 * h), slice(2 * h, 3 * h), slice(0, h), slice(3 * h, 4 * h)
    lefts, rights = slice(0, side), slice(side, 2 * side)
    left_ok, right_ok = col > 0, col < n_col - 1
    pl.when(row == 0)(lambda: fill(R, top_h, every))
    pl.when(row == n_row - 1)(lambda: fill(R, end_h, every))
    pl.when(col == 0)(lambda: fill(R, every, top_h))
    pl.when(col == n_col - 1)(lambda: fill(R, every, end_h))

    barrier = pltpu.get_barrier_semaphore()
    for d in range(1, n_row):
        pl.semaphore_signal(barrier, inc=1, device_id=(lax.rem(row + d, n_row), col), device_id_type=MESH)
    for d in range(1, n_col):
        pl.semaphore_signal(barrier, inc=1, device_id=(row, lax.rem(col + d, n_col)), device_id_type=MESH)
    pl.semaphore_wait(barrier, n_row - 1 + n_col - 1)

    odd = lax.rem(row, 2)
    inner_row = row + 1 - 2 * odd
    outer_row = row - 1 + 2 * odd
    inner_ok = inner_row < n_row
    outer_ok = jnp.logical_and(outer_row >= 0, outer_row < n_row)
    bent = lax.rem((row + 1) // 2, n_x) == 0
    z_first = (jnp.logical_and(bent, outer_ok), outer_ok)
    x_first = tuple(jnp.logical_not(z) for z in z_first)
    x_pair = tuple(jnp.logical_and(x, outer_ok) for x in x_first)

    def band(start, size=h):
        return pl.ds(pl.multiple_of(start, h), size)

    inn, inn_halo, inn_there = band((2 - odd) * h), band(3 * h * (1 - odd)), band(3 * h * odd)
    out, out_halo, out_there = band((1 + odd) * h), band(3 * h * odd), band(3 * h * (1 - odd))
    outer = band(2 * h * odd, side)

    class Swap:
        def __init__(self, sems, parts):
            send, recv = sems
            self.parts = []
            for q, (src, dst, device, sends, gets) in enumerate(parts):
                self.parts.append((pltpu.make_async_remote_copy(
                    src_ref=src, dst_ref=dst, send_sem=send(q), recv_sem=recv(q),
                    device_id=device, device_id_type=MESH), sends, gets))

        def start(self):
            for copy, sends, _ in self.parts:
                pl.when(sends)(copy.start)

        def wait(self):
            for copy, sends, gets in self.parts:
                pl.when(sends)(copy.wait_send)
                pl.when(gets)(copy.wait_recv)

    def once(index):
        return (lambda q: one_send.at[index + q]), (lambda q: one_recv.at[index + q])

    def turn(index, phase):
        return (lambda q: two_send.at[phase, index + q]), (lambda q: two_recv.at[phase, index + q])

    def across(sems, left_src, left_dst, right_src, right_dst, on):
        go_left, go_right = jnp.logical_and(on, left_ok), jnp.logical_and(on, right_ok)
        return Swap(sems, [
            (left_src, left_dst, (row, col - 1), go_left, go_right),
            (right_src, right_dst, (row, col + 1), go_right, go_left)])

    def leftward(sems, src, dst, on):
        return Swap(sems, [(src, dst, (row, col - 1), jnp.logical_and(on, left_ok), jnp.logical_and(on, right_ok))])

    def rightward(sems, src, dst, on):
        return Swap(sems, [(src, dst, (row, col + 1), jnp.logical_and(on, right_ok), jnp.logical_and(on, left_ok))])

    def along(sems, src, dst, there, on, gets=None):
        return Swap(sems, [(src, dst, (there, col), on, on if gets is None else gets)])

    yes = col >= 0

    def spread(F):
        ends = [
            across(once(30 + 2 * c), F.at[c, out, one], F.at[c, out, end_h], F.at[c, out, two], F.at[c, out, top_h], yes)
            for c in range(2)
        ]
        mids = across(once(34), F.at[:, inn, one], F.at[:, inn, end_h], F.at[:, inn, two], F.at[:, inn, top_h], yes)
        firsts = [along(once(36 + c), F.at[c, out, own], F.at[c, out_there, own], outer_row, z_first[c]) for c in range(2)]
        ends[0].start()
        firsts[1].start()
        firsts[0].start()
        mids.start()
        ends[1].start()
        laters = []
        ends[0].wait()
        laters.append(along(once(38), F.at[0, out, :], F.at[0, out_there, :], outer_row, x_pair[0]))
        laters[-1].start()
        for c in (1, 0):
            firsts[c].wait()
            laters.append(across(
                once(40 + 2 * c), F.at[c, out_halo, one], F.at[c, out_halo, end_h],
                F.at[c, out_halo, two], F.at[c, out_halo, top_h], z_first[c]))
            laters[-1].start()
        mids.wait()
        laters.append(along(once(44), F.at[:, inn, :], F.at[:, inn_there, :], inner_row, inner_ok))
        laters[-1].start()
        ends[1].wait()

        def wait():
            for swap in laters:
                swap.wait()

        return wait

    load_r.wait()
    spread_wait = spread(R)

    fill(G, every, every)
    fill(L, every, every)
    for buf in (D, SOL):
        fill(buf, slice(0, buf.shape[1]), slice(0, buf.shape[2]))

    load_p.wait()
    for s in range(cap):
        on = jnp.where(s < cnt_ref[0, 0], 1.0, 0.0).astype(F32)
        for c in range(2):
            rolled = pltpu.roll(P0[c], off_ref[0, s] + h, 0)
            PR[s, c] = pltpu.roll(rolled, off_ref[1, s] + h, 1) * on

    def three(val):
        top = val.astype(BF16)
        rest = val - top.astype(F32)
        mid = rest.astype(BF16)
        return top, mid, (rest - mid.astype(F32)).astype(BF16)

    load_w.wait()
    first = lax.broadcasted_iota(jnp.int32, (side, side), 0)
    second = lax.broadcasted_iota(jnp.int32, (side, side), 1)
    freq = jnp.where(first >= h, 2 * (first - h) + 1, 2 * first)
    pick = jnp.where(second == freq, 1.0, 0.0).astype(BF16)
    by_row = sum(jnp.dot(pick, part, preferred_element_type=F32) for part in three(W0[...]))
    parts = three(by_row)
    lane = jnp.where(second >= h, second - h, second)
    for q in range(2):
        pick = jnp.where(first == 2 * lane + q, 1.0, 0.0).astype(BF16)
        W[q] = sum(jnp.dot(part, pick, preferred_element_type=F32) for part in parts)

    load_m.wait()
    spread_wait()

    step = 32

    def fold(val):
        return jnp.sum(val.reshape(-1, 8, val.shape[-1]), axis=0)

    sub = lax.broadcasted_iota(jnp.int32, (step, h), 0)
    lan = lax.broadcasted_iota(jnp.int32, (step, h), 1)

    def side_of(s, at):
        if s == 0:
            return "both" if at < h else "near"
        if s == 1:
            return "far" if at < h else "both"
        return "both"

    def patch(s, k, seen, acc):
        X, Y = XS[k], YS[k]
        a = off_ref[0, s] + h
        b = off_ref[1, s] + h

        def put(j, rows, val):
            hi = val.astype(BF16)
            X[j, 0, rows, :] = hi
            X[j, 1, rows, :] = (val - hi.astype(F32)).astype(BF16)

        def left(m, j):
            hi, lo = mat_ref[m], mat_ref[m + 1]
            xh, xl = X[j, 0], X[j, 1]
            return jnp.dot(
                jnp.concatenate([hi, lo, hi], 1), jnp.concatenate([xh, xh, xl], 0), preferred_element_type=F32)

        def right(j, m):
            hi, lo = mat_ref[m], mat_ref[m + 1]
            xh, xl = X[j, 0], X[j, 1]
            return jnp.dot(
                jnp.concatenate([xh, xl, xh], 1), jnp.concatenate([hi, hi, lo], 0), preferred_element_type=F32)

        def covered(c, base):
            halves = []
            for at in (0, h):
                cols, fcols = slice(at, at + h), slice(side + at, side + at + h)
                rk, ck = side_of(s, base), side_of(s, at)
                rows, far = slice(base, base + step), slice(side + base, side + base + step)

                def in_cols(r):
                    if ck == "near":
                        return R[c, r, cols]
                    if ck == "far":
                        return R[c, r, fcols]
                    return jnp.where(lan + at >= b, R[c, r, cols], R[c, r, fcols])

                if rk == "near":
                    halves.append(in_cols(rows))
                elif rk == "far":
                    halves.append(in_cols(far))
                else:
                    halves.append(jnp.where(sub + base >= a, in_cols(rows), in_cols(far)))
            return jnp.concatenate(halves, 1)

        def scatter(c, base, term):
            for at in (0, h):
                val = term[:, at:at + h]
                rk, ck = side_of(s, base), side_of(s, at)
                rows = {}
                if rk == "both":
                    near = jnp.where(sub + base >= a, val, 0.0)
                    rows = {0: near, side: val - near}
                else:
                    rows = {0 if rk == "near" else side: val}
                for shift, part in rows.items():
                    if ck == "both":
                        near = jnp.where(lan + at >= b, part, 0.0)
                        cells = {0: near, side: part - near}
                    else:
                        cells = {0 if ck == "near" else side: part}
                    for over, cell in cells.items():
                        r0, c0 = shift + base, over + at
                        where = (c, slice(r0, r0 + step), slice(c0, c0 + h))
                        if (c, r0, c0) in seen:
                            S[where] += cell
                        else:
                            S[where] = cell
                            seen.add((c, r0, c0))

        def load():
            for t in range(0, h, step):
                parts = []
                for base in (t, h + t):
                    rows = slice(base, base + step)
                    v = [covered(c, base) for c in range(2)]
                    p0, p1 = PR[s, 0, rows, :], PR[s, 1, rows, :]
                    parts.append((p0 * v[0] - p1 * v[1], p0 * v[1] + p1 * v[0]))
                for c in range(2):
                    rows = slice(c * h + t, c * h + t + step)
                    put(0, rows, parts[0][c] + parts[1][c])
                    put(1, rows, parts[0][c] - parts[1][c])

        def mul_a():
            Y[0] = left(0, 0)
            Y[1] = left(4, 1)

        def mix_b():
            for j in range(2):
                for t in range(0, h, step):
                    re, im = Y[j, t:t + step, :], Y[j, h + t:h + t + step, :]
                    rows = slice(j * h + t, j * h + t + step)
                    put(2, rows, jnp.concatenate([re[:, :h] + re[:, h:], im[:, :h] + im[:, h:]], 1))
                    put(3, rows, jnp.concatenate([re[:, :h] - re[:, h:], im[:, :h] - im[:, h:]], 1))

        def mul_b():
            Y[2] = right(2, 2)
            Y[3] = right(3, 6)

        def mix_c():
            for j in range(2):
                for t in range(0, side, step):
                    rows = slice(t, t + step)
                    f = Y[2 + j, rows, :]
                    wf = W[j, rows, :] * f
                    acc[0] = acc[0] + fold(wf * f)
                    put(j, rows, wf)

        def mul_c():
            Y[0] = right(0, 0)
            Y[1] = right(1, 4)

        def mix_d():
            for j in range(2):
                for t in range(0, h, step):
                    rows = slice(j * h + t, j * h + t + step)
                    c, d = Y[0, rows, :], Y[1, rows, :]
                    p, m = c + d, c - d
                    put(2 + j, slice(t, t + step), jnp.concatenate([p[:, :h], m[:, :h]], 1))
                    put(2 + j, slice(h + t, h + t + step), jnp.concatenate([p[:, h:], m[:, h:]], 1))

        def mul_d():
            Y[2] = left(2, 2)
            Y[3] = left(6, 3)

        def store():
            for t in range(0, h, step):
                for sign, base in ((1, t), (-1, h + t)):
                    rows = slice(base, base + step)
                    if sign == 1:
                        hr = Y[2, t:t + step, :] + Y[3, t:t + step, :]
                        hi = Y[2, h + t:h + t + step, :] + Y[3, h + t:h + t + step, :]
                    else:
                        hr = Y[2, t:t + step, :] - Y[3, t:t + step, :]
                        hi = Y[2, h + t:h + t + step, :] - Y[3, h + t:h + t + step, :]
                    p0, p1 = PR[s, 0, rows, :], PR[s, 1, rows, :]
                    scatter(0, base, p0 * hr + p1 * hi)
                    scatter(1, base, p0 * hi - p1 * hr)

        return [load, mul_a, mix_b, mul_b, mix_c, mul_c, mix_d, mul_d, store]

    def lanes(acc):
        total = acc[:, 0:128]
        for q in range(128, acc.shape[1], 128):
            total = total + acc[:, q:q + 128]
        return jnp.sum(total, axis=0, keepdims=True)

    def iteration(it, carry):
        alpha_before, rr_before = carry
        last = it + 1 == ITERS

        def norm(i, acc):
            v = R[:, pl.ds(pl.multiple_of(h + i * 32, 32), 32), own]
            return acc + fold(v[0] * v[0]) + fold(v[1] * v[1])
        rr_acc = lax.fori_loop(0, side // 32, norm, jnp.zeros((8, side), F32))

        order = [*range(2, cap), 0, 1]
        seen = set()
        acc = [jnp.zeros((8, side), F32)]
        timed = []
        for n, s in enumerate(order):
            for q, stage in enumerate(patch(s, n, seen, acc)):
                timed.append((SKEW * n + q, n, stage))
        for _, _, stage in sorted(timed, key=lambda x: x[:2]):
            stage()
        acc = acc[0]

        phase = lax.rem(it, 2)
        rr_l, pap_l = lanes(rr_acc), lanes(acc)
        T1[it, row] = jnp.concatenate([rr_l, pap_l + RIDGE * rr_l], 0)
        ones = [
            pltpu.make_async_remote_copy(
                src_ref=T1.at[it, row], dst_ref=T1.at[it, row], send_sem=s1_send.at[it, d],
                recv_sem=s1_recv.at[it, d], device_id=(lax.rem(row + d, n_row), col), device_id_type=MESH)
            for d in range(1, n_row)
        ]
        for copy in ones:
            copy.start()

        more = jnp.logical_not(last)

        def rows_of(ref_rows, at):
            return pl.ds(pl.multiple_of(ref_rows.start + at, 32), 32)

        tall = side // STRIPS

        def strip(q):
            return pl.ds(pl.multiple_of(2 * h * odd + q * tall, tall), tall)

        halves = (lefts, rights)
        pieces = [(c, q) for c in (1, 0) for q in range(STRIPS)]
        fold_z = {
            (c, q): across(
                once(48 + 2 * (c * STRIPS + q)), S.at[c, strip(q), top_h], ZR.at[1, c, q], S.at[c, strip(q), end_h],
                ZR.at[0, c, q], z_first[c])
            for c, q in pieces
        }
        fold_x = {
            (c, p): along(once(8 + 2 * c + p), S.at[c, out_halo, halves[p]], RXO.at[c, p], outer_row, x_pair[c])
            for c in range(1) for p in range(2)
        }
        fold_i = along(once(12), S.at[:, inn_halo, :], RXI, inner_row, inner_ok)
        fold_z[1, 0].start()
        fold_x[0, 0].start()
        fold_x[0, 1].start()
        fold_i.start()
        for key in pieces[1:]:
            fold_z[key].start()

        def meet(index, src, buf, on):
            def slot(p, c0, c1):
                return buf.at[(phase, p) + (slice(None),) * (len(buf.shape) - 3) + (slice(c0, c1),)]

            full, part = jnp.logical_and(on, more), jnp.logical_and(on, last)
            to_left = (
                leftward(turn(index, phase), src(0, side), slot(1, 0, side), full),
                leftward(turn(index, phase), src(0, h), slot(1, 0, h), part))
            to_right = (
                rightward(turn(index + 1, phase), src(side, 2 * side), slot(0, 0, side), full),
                rightward(turn(index + 1, phase), src(3 * h, 4 * h), slot(0, h, side), part))
            return to_left, to_right

        meet_i = meet(0, lambda c0, c1: S.at[:, inn, c0:c1], DXI, yes)
        meet_x = [
            meet(2 + 2 * c, lambda c0, c1, c=c: S.at[c, out, c0:c1], DXO[c], x_first[c]) for c in range(2)
        ]
        meet_z = {
            (c, q): along(
                turn(6 + c * STRIPS + q, phase), S.at[c, strip(q), own], DZ.at[phase, c, q], outer_row,
                jnp.logical_and(z_first[c], jnp.logical_or(more, odd == 2 * q // STRIPS)),
                jnp.logical_and(z_first[c], jnp.logical_or(more, odd != 2 * q // STRIPS)))
            for c, q in pieces
        }

        def begin(pair):
            for swap in pair:
                swap.start()

        def end(pair):
            for swap in pair:
                swap.wait()

        fold_i.wait()

        @pl.when(inner_ok)
        def _():
            def add(at):
                S[:, rows_of(inn, at), :] += RXI[:, pl.ds(at, 32), :]
            chunks(h, 32, add)
        begin(meet_i[0])
        begin(meet_i[1])

        def turn_z(c, q):
            fold_z[c, q].wait()
            for ok, cols, side_q in ((left_ok, one, 0), (right_ok, two, 1)):
                @pl.when(jnp.logical_and(z_first[c], ok))
                def _():
                    def add(at):
                        S[c, rows_of(strip(q), at), cols] += ZR[side_q, c, q, pl.ds(at, 32), :]
                    chunks(tall, 32, add)
            meet_z[c, q].start()

        def turn_x(c):
            for p in range(2):
                if c == 0:
                    fold_x[c, p].wait()

                    @pl.when(x_pair[c])
                    def _():
                        def add(at):
                            S[c, rows_of(out, at), halves[p]] += RXO[c, p, pl.ds(at, 32), :]
                        chunks(h, 32, add)
                begin(meet_x[c][p])

        for copy in ones:
            copy.wait()
        total = T1[it, 0]
        for q in range(1, n_row):
            total = total + T1[it, q]
        T2[it, col] = total
        twos = [
            pltpu.make_async_remote_copy(
                src_ref=T2.at[it, col], dst_ref=T2.at[it, col], send_sem=s2_send.at[it, d],
                recv_sem=s2_recv.at[it, d], device_id=(row, lax.rem(col + d, n_col)), device_id_type=MESH)
            for d in range(1, n_col)
        ]
        for copy in twos:
            copy.start()
        for key in pieces[:STRIPS]:
            turn_z(*key)
        turn_x(0)
        for key in pieces[STRIPS:]:
            turn_z(*key)
        turn_x(1)

        def settle(c, rows, p, got):
            ok, cols, mine = ((left_ok, lefts, one), (right_ok, rights, two))[p]

            @pl.when(ok)
            def _():
                def run(at):
                    here = rows_of(rows, at)
                    G[c, here, cols] = S[c, here, cols] + got(pl.ds(at, 32))
                chunks(h, 32, run)

            @pl.when(jnp.logical_not(ok))
            def _():
                def run(at):
                    here = rows_of(rows, at)
                    G[c, here, mine] = S[c, here, mine]
                chunks(h, 32, run)

        shares = []

        def share(swap):
            swap.start()
            shares.append(swap)

        def done_i(p):
            end(meet_i[1 - p])
            for c in range(2):
                settle(c, inn, p, lambda there, c=c: DXI[phase, p, c, there, :])
            share(along(once(16 + p), G.at[:, inn, halves[p]], G.at[:, inn_there, halves[p]], inner_row,
                        jnp.logical_and(inner_ok, more)))

        def done_x(c, p):
            end(meet_x[c][1 - p])

            @pl.when(x_first[c])
            def _():
                settle(c, out, p, lambda there: DXO[c][phase, p, there, :])
            if c == 0:
                share(along(once(18 + 2 * c + p), G.at[c, out, halves[p]], G.at[c, out_there, halves[p]], outer_row,
                            jnp.logical_and(x_pair[c], more)))

        def done_z(c, q):
            meet_z[c, q].wait()

            @pl.when(z_first[c])
            def _():
                def run(at):
                    here = rows_of(strip(q), at)
                    G[c, here, own] = S[c, here, own] + DZ[phase, c, q, pl.ds(at, 32), :]
                chunks(tall, 32, run)
            share(across(
                once(48 + 4 * STRIPS + 2 * (c * STRIPS + q)), G.at[c, strip(q), one], G.at[c, strip(q), end_h],
                G.at[c, strip(q), two], G.at[c, strip(q), top_h], jnp.logical_and(z_first[c], more)))

        for key in pieces[:STRIPS]:
            done_z(*key)
        done_i(0)
        done_i(1)
        done_x(0, 0)
        done_x(0, 1)
        for key in pieces[STRIPS:]:
            done_z(*key)
        done_x(1, 0)
        done_x(1, 1)

        for copy in twos:
            copy.wait()
        total = T2[it, 0]
        for q in range(1, n_col):
            total = total + T2[it, q]
        rr = jnp.sum(total[0:1], keepdims=True)
        pap = jnp.sum(total[1:2], keepdims=True)
        ratio = jnp.where(it == 0, 0.0, rr / rr_before)
        alpha = rr / (pap - ratio * rr / alpha_before)

        def update(rows, cols):
            for c in range(2):
                r = R[c, rows, cols]
                image = G[c, rows, cols] + RIDGE * r + ratio * L[c, rows, cols]
                L[c, rows, cols] = image
                R[c, rows, cols] = r - alpha * image

        def advance(i, carry):
            near = pl.ds(pl.multiple_of(i * 32, 32), 32)
            rows = pl.ds(pl.multiple_of(h + i * 32, 32), 32)
            for c in range(2):
                d = R[c, rows, own] + ratio * D[c, near, :]
                D[c, near, :] = d
                SOL[c, near, :] += alpha * d
            return carry
        lax.fori_loop(0, side // 32, advance, 0)

        @pl.when(more)
        def _():
            def advance_own(at):
                rows = pl.ds(pl.multiple_of(h + at, 32), 32)
                update(rows, own)
            chunks(side, 32, advance_own)
        for swap in shares:
            swap.wait()

        @pl.when(more)
        def _():
            def advance_r(at):
                update(pl.ds(pl.multiple_of(at, 32), 32), every)
                update(pl.ds(pl.multiple_of(3 * h + at, 32), 32), every)
                for shift in (h, 2 * h):
                    update(pl.ds(pl.multiple_of(shift + at, 32), 32), top_h)
                    update(pl.ds(pl.multiple_of(shift + at, 32), 32), end_h)
            chunks(h, 32, advance_r)

        @pl.when(last)
        def _():
            def emit(at):
                rows = pl.ds(pl.multiple_of(h + at, 32), 32)
                for c in range(2):
                    r = R[c, rows, own]
                    image = G[c, rows, own] + RIDGE * r + ratio * L[c, rows, own]
                    res_ref[c, pl.ds(at, 32), :] = r - alpha * image
            chunks(side, 32, emit)
        return alpha, rr

    one11 = jnp.ones((1, 1), F32)
    lax.fori_loop(0, ITERS, iteration, (one11, one11))


def solution(mesh):
    n_row, n_col = mesh.shape["row"], mesh.shape["col"]
    n_x = len({tuple(getattr(d, "coords", (d.id,)))[0] for d in mesh.devices.flat})

    def local(right_side, probe, weights, offsets, counts):
        side = probe.shape[1]
        cap = offsets.shape[2]
        h = side // 2
        mats = jnp.asarray(tables(side))
        weights = pltpu.with_memory_space_constraint(weights, pltpu.HBM)
        block = jax.ShapeDtypeStruct((2, side, side), F32)
        hbm = pl.BlockSpec(memory_space=pltpu.HBM)
        smem = pl.BlockSpec(memory_space=pltpu.SMEM)
        wide = pltpu.VMEM((2, 2 * side, 2 * side), F32)
        tile = pltpu.VMEM((2, side, side), F32)
        dma = pltpu.SemaphoreType.DMA
        vmem = pl.BlockSpec(memory_space=pltpu.VMEM)
        return pl.pallas_call(
            functools.partial(kernel, n_row, n_col, n_x, cap, side),
            out_shape=(block, block),
            in_specs=[smem, smem, hbm, hbm, hbm, hbm],
            out_specs=(vmem, vmem),
            scratch_shapes=[
                wide, wide, wide, wide,
                tile,
                pltpu.VMEM((cap, 2, side, side), F32),
                tile,
                pltpu.VMEM((side, side), F32),
                pltpu.VMEM((8, side, side), BF16),
                [pltpu.VMEM((4, 2, side, side), BF16) for _ in range(cap)],
                [pltpu.VMEM((4, side, side), F32) for _ in range(cap)],
                tile,
                pltpu.VMEM((2, h, 2 * side), F32),
                pltpu.VMEM((2, 2, h, side), F32),
                pltpu.VMEM((2, 2, 2, h, side), F32),
                [pltpu.VMEM((2, 2, h, side), F32) for _ in range(2)],
                pltpu.VMEM((2, 2, STRIPS, side // STRIPS, h), F32),
                pltpu.VMEM((2, 2, STRIPS, side // STRIPS, side), F32),
                pltpu.VMEM((ITERS, n_row, 2, 128), F32),
                pltpu.VMEM((ITERS, n_col, 2, 128), F32),
                dma((48 + 8 * STRIPS,)), dma((48 + 8 * STRIPS,)), dma((2, 6 + 2 * STRIPS)), dma((2, 6 + 2 * STRIPS)),
                dma((ITERS, n_row)), dma((ITERS, n_row)),
                dma((ITERS, n_col)), dma((ITERS, n_col)),
                dma((4,)),
            ],
            compiler_params=pltpu.CompilerParams(
                collective_id=0, has_side_effects=True, vmem_limit_bytes=53824 * 1024),
        )(pltpu.with_memory_space_constraint(offsets[0, 0].T, pltpu.HBM), counts, right_side, probe, weights, mats)

    placed = (P(None, "row", "col"), P(), P(), P("row", "col", None, None), P("row", "col"))
    return jax.shard_map(
        local, mesh=mesh, in_specs=placed, out_specs=(P(None, "row", "col"), P(None, "row", "col")), check_vma=False)
```
